512 devices in a mesh: groups: 2 (over y), dp: 128 (over z, x), tp: 2 (over core).
Axes of the slice: x: 8, y: 2, z: 16, core: 2. Of those that a mesh axis runs over, the one named last changes fastest.
The devices are a block of a 8x8x16 slice.
Arguments:
- pool: bfloat16 [32768, 4608], P(('groups', 'dp')), parts along dimension 0, may hold values from -10 to 10
- page_holder: int32 [14336], P(('groups', 'dp')), parts along dimension 0, may hold values from 0 to 127, as said below
- page_slot: int32 [14336], P(('groups', 'dp')), parts along dimension 0, may hold values from 0 to 127
- suffix_latent_rows: bfloat16 [256, 9216], P(('groups', 'dp')), parts along dimension 0, may hold values from -5 to 5
- prefill_queries: bfloat16 [256, 128, 4608], P(('groups', 'dp'), None, 'tp'), parts along dimension 0, may hold values from -10 to 10
- suffix_len: int32 [32], P('groups'), parts along dimension 0, may hold values from 1 to 128
- decode_queries: bfloat16 [1024, 36864], P(('groups', 'dp'), 'tp'), parts along dimension 0, may hold values from -10 to 10
- decode_len: int32 [1024], P(('groups', 'dp')), parts along dimension 0, may hold values from 1 to 256
Outputs:
- prefill_output: bfloat16 [256, 128, 4096], P(('groups', 'dp'), None, 'tp'), parts along dimension 0
- decode_out: bfloat16 [1024, 32768], P(('groups', 'dp'), 'tp'), parts along dimension 0
The draws below stay inside these ranges and needn't reach their ends.
There are 2 independent parts, one for each index of `groups`. The reference program is written for one: setup_inputs(seed, part) draws one part's arguments, and reference() takes and returns one part's arrays. A program takes and returns all parts, laid end to end along the dimension named above; each array names one. Nothing has to cross between parts.
Inputs may be any that keep to these rules, and one draw needn't show every extreme that they name: `page_holder`: within one device's 56 entries no holder appears more than 1 times, and some holder appears exactly 1 times.
All inputs are finite; a program needn't handle non-finite values.
Results may differ from the reference program's by a relative error of at most 0.004.
Values may be sent and summed in bfloat16 or wider, within the bound.
A program may use at most 64 MiB of HBM per device.

```python
import jax
import jax.numpy as jnp
from jax import lax

ATTENTION_HEADS = 64
LATENT_WIDTH = 512
ROTARY_WIDTH = 64
PAGE_TOKENS = 8
SUFFIX_SHARE = 16
TEAM_RANKS = 8
PULL = 56
DECODE_ROWS_DP = 4
ROW_PAGES = 32
POOL_PAGES = 128
SUFFIX_TOKENS = 128
N_DP = 128


def query_block(key, leading, spread):
    compressed_width = LATENT_WIDTH + ROTARY_WIDTH
    drawn = jax.random.normal(jax.random.fold_in(key, 15), leading + (compressed_width,), jnp.float32) * spread
    return jnp.clip(drawn, -4.0 * spread, 4.0 * spread)


def draw_pool(key, part):
    row_count = N_DP * POOL_PAGES
    compressed_width = LATENT_WIDTH + ROTARY_WIDTH
    base_key = jax.random.fold_in(key, 4201)
    value_rows = jnp.clip(jax.random.normal(base_key, (row_count, PAGE_TOKENS, compressed_width), jnp.float32), -4.0, 4.0)
    return value_rows.reshape(row_count, PAGE_TOKENS * compressed_width).astype(jnp.bfloat16)


def draw_page_holder(key, part):
    subkeys = jax.random.split(jax.random.fold_in(key, 5303), N_DP)

    def draw_order(subkey):
        return jax.random.permutation(subkey, N_DP)
    orders = jax.vmap(draw_order)(subkeys)
    picks = jnp.arange(PULL, dtype=jnp.int32) % N_DP
    return orders[:, picks].reshape(N_DP * PULL).astype(jnp.int32)


def draw_prefill_queries(key, part):
    value_rows = query_block(jax.random.fold_in(key, 6101), (N_DP, SUFFIX_TOKENS, ATTENTION_HEADS // TEAM_RANKS), 1.4)
    return value_rows.reshape(N_DP, SUFFIX_TOKENS, ATTENTION_HEADS // TEAM_RANKS * (LATENT_WIDTH + ROTARY_WIDTH)).astype(jnp.bfloat16)


def draw_decode_queries(key, part):
    value_rows = query_block(jax.random.fold_in(key, 6202), (N_DP * DECODE_ROWS_DP, ATTENTION_HEADS), 1.0)
    return value_rows.reshape(N_DP * DECODE_ROWS_DP, ATTENTION_HEADS * (LATENT_WIDTH + ROTARY_WIDTH)).astype(jnp.bfloat16)


def place_ends(values, stream_key, least, high):
    place = [jax.random.randint(jax.random.fold_in(stream_key, axis), (), 0, length) for axis, length in enumerate(values.shape)]
    main_axis = values.shape.index(max(values.shape))
    beside = place[:main_axis] + [(place[main_axis] + 1) % values.shape[main_axis]] + place[main_axis + 1:]
    return values.at[tuple(place)].set(least).at[tuple(beside)].set(high)


def shard_levels(stream_key, shape, cuts, smallest, largest):
    level, own = 1.0, jax.random.fold_in(stream_key, 6)
    for axis_at, shards_of in cuts:
        steps = jnp.exp(jax.random.uniform(jax.random.fold_in(own, axis_at), (shards_of,), jnp.float32, smallest / len(cuts), largest / len(cuts)))
        level = level * jnp.repeat(steps, shape[axis_at] // shards_of).reshape([-1 if axis == axis_at else 1 for axis in range(len(shape))])
    return level


def noise(key, extent, deviation, limit, cuts=(), kind=jnp.bfloat16):
    entries = jax.random.normal(key, extent, jnp.float32) * deviation
    if len(cuts) > 0:
        entries = shard_levels(key, extent, cuts, -0.22, 0.18) * entries
    return jnp.clip(entries, min=-limit, max=limit).astype(kind)


def setup_inputs(seed: int = 0, part: int = 0) -> dict:
    key_list = jax.random.split(jax.random.key(seed), 9)
    part_keys = jax.random.split(jax.random.fold_in(key_list[8], part), 9)
    pool = draw_pool(jax.random.fold_in(jax.random.fold_in(key_list[8], part), 71), part)
    page_holder = draw_page_holder(jax.random.fold_in(jax.random.fold_in(key_list[8], part), 71), part)
    page_slot = place_ends(jax.random.randint(part_keys[2], (N_DP * PULL,), 0, POOL_PAGES), jax.random.fold_in(part_keys[2], 1), 0, POOL_PAGES - 1).astype(jnp.int32)
    suffix_latent_rows = noise(part_keys[3], (N_DP, SUFFIX_SHARE * (LATENT_WIDTH + ROTARY_WIDTH)), 1.25, 5.0, ((0, 128),))
    prefill_queries = draw_prefill_queries(jax.random.fold_in(jax.random.fold_in(key_list[8], part), 71), part)
    suffix_len = place_ends(jax.random.randint(part_keys[5], (N_DP // TEAM_RANKS,), 1, SUFFIX_TOKENS + 1), jax.random.fold_in(part_keys[5], 1), 1, SUFFIX_TOKENS).astype(jnp.int32)
    decode_queries = draw_decode_queries(jax.random.fold_in(jax.random.fold_in(key_list[8], part), 71), part)
    decode_len = place_ends(jax.random.randint(part_keys[7], (N_DP * DECODE_ROWS_DP,), 1, ROW_PAGES * PAGE_TOKENS + 1), jax.random.fold_in(part_keys[7], 1), 1, ROW_PAGES * PAGE_TOKENS).astype(jnp.int32)
    return dict(pool=pool, page_holder=page_holder, page_slot=page_slot, suffix_latent_rows=suffix_latent_rows, prefill_queries=prefill_queries, suffix_len=suffix_len, decode_queries=decode_queries, decode_len=decode_len)


softmax_scale = 192.0 ** -0.5
masked_score = -1.0e30


def attend_rows(queries, key_matrix, allowed):
    scores = jnp.einsum('shr,kr->shk', queries.astype(jnp.float32), key_matrix.astype(jnp.float32)) * softmax_scale
    scores = jnp.where(allowed[:, None, :], scores, masked_score)
    row_peak = jnp.max(scores, axis=-1, keepdims=True)
    powers = jnp.exp(scores - row_peak)
    denominator = jnp.sum(powers, axis=-1)
    weights = powers.astype(jnp.bfloat16)
    value_rows = key_matrix[:, :LATENT_WIDTH]
    blended_output = jnp.einsum('shk,kc->shc', weights.astype(jnp.float32), value_rows.astype(jnp.float32))
    return blended_output / denominator[..., None]


def reference(pool, page_holder, page_slot, suffix_latent_rows, prefill_queries, suffix_len, decode_queries, decode_len):
    compressed_width = LATENT_WIDTH + ROTARY_WIDTH
    team_heads = ATTENTION_HEADS // TEAM_RANKS
    requests = N_DP // TEAM_RANKS
    holders = page_holder.reshape(requests, TEAM_RANKS * PULL)
    slot_table = page_slot.reshape(requests, TEAM_RANKS * PULL)
    suffixes = suffix_latent_rows.reshape(requests, SUFFIX_TOKENS, compressed_width)
    queries = prefill_queries.reshape(requests, TEAM_RANKS, SUFFIX_TOKENS, team_heads, compressed_width)
    positions = jnp.arange(SUFFIX_TOKENS, dtype=jnp.int32)
    prefix_count = TEAM_RANKS * PULL * PAGE_TOKENS

    def one_request(request_no):
        page_rows = pool[holders[request_no] * POOL_PAGES + slot_table[request_no]]
        key_matrix = jnp.concatenate([page_rows.reshape(prefix_count, compressed_width), suffixes[request_no]], axis=0)
        length = suffix_len[request_no]
        prefix_ok = jnp.ones((SUFFIX_TOKENS, prefix_count), dtype=bool)
        suffix_ok = (positions[None, :] <= positions[:, None]) & (positions[None, :] < length)
        allowed = jnp.concatenate([prefix_ok, suffix_ok], axis=1)

        def one_member(member_queries):
            return attend_rows(member_queries, key_matrix, allowed)

        blended_output = lax.map(one_member, queries[request_no])
        live_rows = positions < length
        blended_output = jnp.where(live_rows[None, :, None, None], blended_output, 0.0)
        return blended_output.reshape(TEAM_RANKS, SUFFIX_TOKENS, team_heads * LATENT_WIDTH).astype(jnp.bfloat16)

    prefill_output = lax.map(one_request, jnp.arange(requests, dtype=jnp.int32))
    prefill_output = prefill_output.reshape(N_DP, SUFFIX_TOKENS, team_heads * LATENT_WIDTH)

    contexts = pool.reshape(N_DP * DECODE_ROWS_DP, ROW_PAGES * PAGE_TOKENS, compressed_width)
    decode_rows = decode_queries.reshape(N_DP * DECODE_ROWS_DP, 1, ATTENTION_HEADS, compressed_width)
    key_positions = jnp.arange(ROW_PAGES * PAGE_TOKENS, dtype=jnp.int32)

    def one_row(items):
        row_queries, context_output, length = items
        allowed = (key_positions < length)[None, :]
        blended_output = attend_rows(row_queries, context_output, allowed)
        return blended_output.reshape(ATTENTION_HEADS * LATENT_WIDTH).astype(jnp.bfloat16)

    decode_out = lax.map(one_row, (decode_rows, contexts, decode_len))
    return prefill_output, decode_out
```

```python
import functools
import math

import jax
import jax.numpy as jnp
from jax import lax
from jax.experimental import pallas as pl
from jax.experimental.pallas import tpu as pltpu
from jax.sharding import Mesh
from jax.sharding import PartitionSpec as P

LATENT_WIDTH = 512
ROTARY_WIDTH = 64
KEY = LATENT_WIDTH + ROTARY_WIDTH
PAIR = 2 * KEY
WIDE = LATENT_WIDTH + 2 * ROTARY_WIDTH
LANES = 128
TEAM_RANKS = 8
GROUPS_DP = ("groups", "dp_0", "dp_1")
MESH_ID = pl.DeviceIdType.MESH

log2_scale = 192.0 ** (-0.5) * math.log2(math.e)
masked_score = -1e30


def dot(a, b):
    return jnp.dot(a, b, preferred_element_type=jnp.float32)


def dot_t(a, b):
    return lax.dot_general(a, b, (((1,), (1,)), ((), ())), preferred_element_type=jnp.float32)


def iota(shape, dim):
    return lax.broadcasted_iota(jnp.int32, shape, dim)


def gather_kernel(
    Z,
    X,
    pool_ref,
    req_ref,
    sel_ref,
    suffix_ref,
    keys_ref,
    suf_ref,
    half_ref,
    c_ref,
    t_ref,
    w_ref,
    sendz,
    recvz,
    sendx,
    recvx,
    pool_sem,
    c_send,
    c_recv,
    w_send,
    w_recv,
    s_send,
    s_recv,
    z_send,
    z_recv,
    x_send,
    x_recv,
    r_send,
    r_recv,
    l_send,
    l_recv,
    d_send,
    d_recv,
):
    my_z = lax.axis_index("dp_0")
    my_x = lax.axis_index("dp_1")
    my_c = lax.axis_index("tp")
    half = half_ref.shape[1]
    right_hops = X // 2
    left_hops = X - 1 - right_hops
    zs = list(range(1, Z))
    xs = list(range(1, X))

    def at_z(d):
        return {"dp_0": lax.rem(my_z + d + Z, Z)}

    def at_x(e):
        return {"dp_1": lax.rem(my_x + e + X, X)}

    sibling = {"tp": 1 - my_c}

    def remote(src, dst, send, recv, where):
        return pltpu.make_async_remote_copy(
            src_ref=src, dst_ref=dst, send_sem=send, recv_sem=recv, device_id=where, device_id_type=MESH_ID
        )

    barrier = pltpu.get_barrier_semaphore()
    for d in zs:
        pl.semaphore_signal(barrier, inc=1, device_id=at_z(d), device_id_type=MESH_ID)
    for e in xs:
        pl.semaphore_signal(barrier, inc=1, device_id=at_x(e), device_id_type=MESH_ID)
    pl.semaphore_signal(barrier, inc=1, device_id=sibling, device_id_type=MESH_ID)
    start = pl.multiple_of(my_c * half, LANES)
    load = pltpu.make_async_copy(pool_ref.at[:, pl.ds(start, half)], half_ref, pool_sem)
    load.start()
    pl.semaphore_wait(barrier, len(zs) + len(xs) + 1)

    c_copies = [remote(req_ref, c_ref.at[e], c_send.at[e], c_recv.at[e], at_x(-e)) for e in xs]
    for copy in c_copies:
        copy.start()
    s_copies = [remote(suffix_ref, suf_ref.at[e], s_send.at[e], s_recv.at[e], at_x(e)) for e in xs]
    for copy in s_copies:
        copy.start()
    suf_ref[0] = suffix_ref[...]
    for copy in c_copies:
        copy.wait_recv()
    rows = [req_ref[...]] + [c_ref[e] for e in xs]
    c_all = jnp.concatenate(rows + [jnp.zeros((LANES - X, LANES), jnp.float32)], axis=0)
    lane = iota((LANES, LANES), 1)
    row = iota((LANES, LANES), 0)
    c_mine = jnp.where(lane // Z == row, c_all, 0.0).astype(jnp.bfloat16)
    pick = (iota((Z, LANES), 1) % Z == iota((Z, LANES), 0)).astype(jnp.bfloat16)
    table = dot_t(pick, c_mine)
    for d in range(Z):
        t_ref[d] = table[d : d + 1, :]

    w_copies = [remote(t_ref.at[d], w_ref.at[d], w_send.at[d], w_recv.at[d], at_z(-d)) for d in zs]
    for copy in w_copies:
        copy.start()
    w_ref[0] = t_ref[0]
    load.wait()
    for copy in w_copies:
        copy.wait_recv()
    spread = jnp.concatenate([jnp.broadcast_to(w_ref[d], (X, LANES)) for d in range(Z)], axis=0)
    lane_g = iota((Z * X, LANES), 1)
    row_g = iota((Z * X, LANES), 0)
    wanted = jnp.sum(jnp.where(lane_g == row_g % X, spread, 0.0), axis=1, keepdims=True).astype(jnp.int32)
    pages = pool_ref.shape[0]
    gather = (wanted == iota((Z * X, pages), 1) + 1).astype(jnp.bfloat16)

    z_copies = []
    for j in range(2):
        taken = dot(gather, half_ref[:, j * PAIR : (j + 1) * PAIR])
        sendz[j] = taken.reshape(Z, X, PAIR).astype(jnp.bfloat16)
        copies = [remote(sendz.at[j, d], recvz.at[j, d], z_send.at[j, d], z_recv.at[j, d], at_z(d)) for d in zs]
        for copy in copies:
            copy.start()
        recvz[j, 0] = sendz[j, 0]
        z_copies.append(copies)

    turn = (
        (iota((X * Z, Z * X), 1) % X == iota((X * Z, Z * X), 0) // Z)
        & (iota((X * Z, Z * X), 1) // X == iota((X * Z, Z * X), 0) % Z)
    ).astype(jnp.bfloat16)
    ended = []
    for j in range(2):
        for copy in z_copies[j]:
            copy.wait_recv()
        arrived = recvz[j].astype(jnp.float32).reshape(Z * X, PAIR).astype(jnp.bfloat16)
        turned = dot(turn, arrived)
        sendx[j] = turned.reshape(X, Z, PAIR).astype(jnp.bfloat16)
        x_copies = [remote(sendx.at[j, e], recvx.at[j, e], x_send.at[j, e], x_recv.at[j, e], at_x(e)) for e in xs]
        for copy in x_copies:
            copy.start()
        recvx[j, 0] = sendx[j, 0]
        for copy in x_copies:
            copy.wait_recv()
        arrived = recvx[j].astype(jnp.float32).reshape(X * Z, PAIR).astype(jnp.bfloat16)
        own = dot(sel_ref[:, : X * Z], arrived).astype(jnp.bfloat16)
        keys_ref[j, 0] = own

        def to_right(i, j=j):
            return remote(keys_ref.at[j, i - 1], keys_ref.at[j, i], r_send.at[j, i], r_recv.at[j, i], at_x(1))

        def to_left(i, j=j):
            return remote(
                keys_ref.at[j, (X - i + 1) % X], keys_ref.at[j, X - i], l_send.at[j, i], l_recv.at[j, i], at_x(-1)
            )

        def across(s, j=j):
            return remote(keys_ref.at[j, s], keys_ref.at[2 + j, s], d_send.at[j, s], d_recv.at[j, s], sibling)

        started = []

        def go(copy):
            copy.start()
            started.append(copy)

        go(to_right(1))
        go(to_left(1))
        crossing = [across(0)]
        crossing[0].start()
        for i in range(1, right_hops + 1):
            to_right(i).wait_recv()
            if i < right_hops:
                go(to_right(i + 1))
            crossing.append(across(i))
            crossing[-1].start()
            if i <= left_hops:
                to_left(i).wait_recv()
                if i < left_hops:
                    go(to_left(i + 1))
                crossing.append(across(X - i))
                crossing[-1].start()
        ended.append((x_copies, started, crossing))

    for copy in c_copies + w_copies + z_copies[0] + z_copies[1]:
        copy.wait_send()
    for copy in s_copies:
        copy.wait()
    for x_copies, started, crossing in ended:
        for copy in x_copies + started:
            copy.wait_send()
        for copy in crossing:
            copy.wait()


def gather_keys(pool, req, sel, suffix, Z, X):
    pages = pool.shape[0]
    pull = sel.shape[0]
    half = pool.shape[1] // 2
    vmem = pl.BlockSpec(memory_space=pltpu.VMEM)
    dma = pltpu.SemaphoreType.DMA
    right_hops = X // 2
    return pl.pallas_call(
        functools.partial(gather_kernel, Z, X),
        out_shape=(
            jax.ShapeDtypeStruct((4, X, pull, PAIR), jnp.bfloat16),
            jax.ShapeDtypeStruct((X, *suffix.shape), jnp.bfloat16),
        ),
        in_specs=[pl.BlockSpec(memory_space=pl.ANY), vmem, vmem, vmem],
        out_specs=(vmem, vmem),
        scratch_shapes=[
            pltpu.VMEM((pages, half), jnp.bfloat16),
            pltpu.VMEM((X, 1, LANES), jnp.float32),
            pltpu.VMEM((Z, 1, LANES), jnp.float32),
            pltpu.VMEM((Z, 1, LANES), jnp.float32),
            pltpu.VMEM((2, Z, X, PAIR), jnp.bfloat16),
            pltpu.VMEM((2, Z, X, PAIR), jnp.bfloat16),
            pltpu.VMEM((2, X, Z, PAIR), jnp.bfloat16),
            pltpu.VMEM((2, X, Z, PAIR), jnp.bfloat16),
            dma,
            dma((X,)),
            dma((X,)),
            dma((Z,)),
            dma((Z,)),
            dma((X,)),
            dma((X,)),
            dma((2, Z)),
            dma((2, Z)),
            dma((2, X)),
            dma((2, X)),
            dma((2, right_hops + 1)),
            dma((2, right_hops + 1)),
            dma((2, right_hops + 1)),
            dma((2, right_hops + 1)),
            dma((2, X)),
            dma((2, X)),
        ],
        compiler_params=pltpu.CompilerParams(collective_id=0, has_side_effects=True),
        name="gather_keys",
    )(pool, req, sel, suffix)


def both_forms(low, high):
    low_lane = iota(low.shape, 1)
    low = jnp.where(low_lane < KEY, low.astype(jnp.float32), 0.0)
    high = jnp.where(low_lane >= ROTARY_WIDTH, high.astype(jnp.float32), 0.0)
    low_moved = pltpu.roll(low, ROTARY_WIDTH, 1)
    high_moved = pltpu.roll(high, WIDE - ROTARY_WIDTH, 1)
    cast = lambda a: a.astype(jnp.bfloat16)
    return cast(low), cast(low_moved), cast(high_moved), cast(high)


def finish(acc_first, acc_second, denominator):
    moved = pltpu.roll(acc_second, WIDE - ROTARY_WIDTH, 1)
    return (acc_first + moved[:, :LATENT_WIDTH]) / denominator


def prefill_kernel(X, len_ref, q_ref, keys_ref, suf_ref, out_ref, q_first, q_second):
    tokens = q_ref.shape[0]
    heads = q_ref.shape[1] // KEY
    my_x = lax.axis_index("dp_1")
    length = len_ref[0]
    for hp in range(heads // 2):
        low = q_ref[:, hp * PAIR : hp * PAIR + WIDE]
        high = q_ref[:, hp * PAIR + LATENT_WIDTH : (hp + 1) * PAIR]
        first_low, second_low, first_high, second_high = both_forms(low, high)
        q_first[2 * hp] = first_low
        q_second[2 * hp] = second_low
        q_first[2 * hp + 1] = first_high
        q_second[2 * hp + 1] = second_high

    block = 2
    share = suf_ref.shape[0] // X

    def step(b, _):
        rows = block * tokens
        queries = [
            q_first[pl.ds(b * block, block)].reshape(rows, WIDE),
            q_second[pl.ds(b * block, block)].reshape(rows, WIDE),
        ]
        pieces = []
        for par in range(2):
            s = dot_t(queries[par], suf_ref[:, par * LATENT_WIDTH : par * LATENT_WIDTH + WIDE]) * log2_scale
            lane = iota(s.shape, 1)
            token = iota(s.shape, 0) % tokens
            rank = lax.rem(my_x - lane // share + X, X)
            pos = rank * (2 * share) + 2 * (lane % share) + par
            pieces.append(jnp.where((pos <= token) & (pos < length), s, masked_score))
        for p in range(keys_ref.shape[0]):
            for par in range(2):
                k = keys_ref[p, :, par * LATENT_WIDTH : par * LATENT_WIDTH + WIDE]
                pieces.append(dot_t(queries[par], k) * log2_scale)
        peak = functools.reduce(jnp.maximum, [jnp.max(s, axis=1, keepdims=True) for s in pieces])
        total = jnp.zeros((rows, 1), jnp.float32)
        acc = [jnp.zeros((rows, LATENT_WIDTH), jnp.float32), jnp.zeros((rows, WIDE), jnp.float32)]
        for n, s in enumerate(pieces):
            par = n % 2
            powers = jnp.exp2(s - peak)
            total = total + jnp.sum(powers, axis=1, keepdims=True)
            width = LATENT_WIDTH if par == 0 else WIDE
            source = suf_ref if n < 2 else keys_ref.at[n // 2 - 1]
            v = source[:, par * LATENT_WIDTH : par * LATENT_WIDTH + width]
            acc[par] = acc[par] + dot(powers.astype(jnp.bfloat16), v)
        result = finish(acc[0], acc[1], total)
        token = iota(result.shape, 0) % tokens
        result = jnp.where(token < length, result, 0.0).astype(jnp.bfloat16)
        for h in range(block):
            at = pl.multiple_of((b * block + h) * LATENT_WIDTH, LANES)
            out_ref[:, pl.ds(at, LATENT_WIDTH)] = result[h * tokens : (h + 1) * tokens]
        return 0

    lax.fori_loop(0, heads // block, step, 0)


def prefill(length, queries, keys, suffix, X):
    tokens = queries.shape[0]
    heads = queries.shape[1] // KEY
    vmem = pl.BlockSpec(memory_space=pltpu.VMEM)
    return pl.pallas_call(
        functools.partial(prefill_kernel, X),
        out_shape=jax.ShapeDtypeStruct((tokens, heads * LATENT_WIDTH), jnp.bfloat16),
        in_specs=[pl.BlockSpec(memory_space=pltpu.SMEM), vmem, vmem, vmem],
        out_specs=vmem,
        scratch_shapes=[
            pltpu.VMEM((heads, tokens, WIDE), jnp.bfloat16),
            pltpu.VMEM((heads, tokens, WIDE), jnp.bfloat16),
        ],
        name="prefill",
    )(length, queries, keys, suffix)


def decode_kernel(len_ref, q_ref, pool_ref, out_ref):
    decode_rows = len_ref.shape[0]
    pages = pool_ref.shape[0]
    row_pages = pages // decode_rows
    head_pairs = q_ref.shape[0] // decode_rows
    first_low, second_low, first_high, second_high = both_forms(q_ref[:, :WIDE], q_ref[:, LATENT_WIDTH:])
    queries = [
        jnp.concatenate([first_low, first_high], axis=0),
        jnp.concatenate([second_low, second_high], axis=0),
    ]
    count = 2 * q_ref.shape[0]
    page = iota((count, pages), 1)
    owner = (iota((count, pages), 0) % q_ref.shape[0]) // head_pairs
    limit = jnp.zeros((count, pages), jnp.int32)
    for r in range(decode_rows):
        limit = jnp.where(owner == r, len_ref[r], limit)
    limit = jnp.where(page // row_pages == owner, limit, 0)
    page_tokens = pool_ref.shape[1] // KEY
    pieces = []
    for n in range(page_tokens):
        at = (n // 2) * PAIR + (n % 2) * LATENT_WIDTH
        s = dot_t(queries[n % 2], pool_ref[:, at : at + WIDE]) * log2_scale
        pieces.append(jnp.where((page % row_pages) * page_tokens + n < limit, s, masked_score))
    peak = functools.reduce(jnp.maximum, [jnp.max(s, axis=1, keepdims=True) for s in pieces])
    total = jnp.zeros((count, 1), jnp.float32)
    acc = [jnp.zeros((count, LATENT_WIDTH), jnp.float32), jnp.zeros((count, WIDE), jnp.float32)]
    for n in range(page_tokens):
        at = (n // 2) * PAIR + (n % 2) * LATENT_WIDTH
        width = LATENT_WIDTH if n % 2 == 0 else WIDE
        powers = jnp.exp2(pieces[n] - peak)
        total = total + jnp.sum(powers, axis=1, keepdims=True)
        acc[n % 2] = acc[n % 2] + dot(powers.astype(jnp.bfloat16), pool_ref[:, at : at + width])
    result = finish(acc[0], acc[1], total).astype(jnp.bfloat16)
    out_ref[:, :LATENT_WIDTH] = result[: count // 2]
    out_ref[:, LATENT_WIDTH:] = result[count // 2 :]


def decode(pool, decode_queries, decode_len):
    decode_rows = decode_queries.shape[0]
    queries = decode_queries.reshape(-1, PAIR)
    vmem = pl.BlockSpec(memory_space=pltpu.VMEM)
    out = pl.pallas_call(
        decode_kernel,
        out_shape=jax.ShapeDtypeStruct((queries.shape[0], 2 * LATENT_WIDTH), jnp.bfloat16),
        in_specs=[pl.BlockSpec(memory_space=pltpu.SMEM), vmem, vmem],
        out_specs=vmem,
        name="decode",
    )(decode_len, queries, pool)
    return out.reshape(decode_rows, -1)


def shards(
    Z,
    X,
    pool,
    page_holder,
    page_slot,
    suffix_latent_rows,
    prefill_queries,
    suffix_len,
    decode_queries,
    decode_len,
):
    my_z = lax.axis_index("dp_0")
    my_x = lax.axis_index("dp_1")
    d = (my_z - page_holder // X) % Z
    e = (my_x - page_holder % X) % X
    chosen = (e * Z + d)[:, None] == jnp.arange(LANES, dtype=jnp.int32)[None, :]
    req = jnp.sum(jnp.where(chosen, page_slot[:, None] + 1, 0), axis=0)[None, :].astype(jnp.float32)
    sel = chosen.astype(jnp.bfloat16)
    suffix = suffix_latent_rows.reshape(-1, PAIR)
    keys, suf = gather_keys(pool, req, sel, suffix, Z, X)
    decode_part = decode(pool, decode_queries, decode_len)
    length = lax.dynamic_slice_in_dim(suffix_len, my_z, 1)
    keys = keys.reshape(keys.shape[0], -1, PAIR)
    suf = suf.reshape(-1, PAIR)
    prefill_part = prefill(length, prefill_queries[0], keys, suf, X)
    return (prefill_part[None], decode_part)


def solution(mesh):
    groups, dp, tp = (mesh.shape[name] for name in ("groups", "dp", "tp"))
    X = TEAM_RANKS
    Z = dp // X
    torus = Mesh(mesh.devices.reshape(groups, Z, X, tp), ("groups", "dp_0", "dp_1", "tp"))
    placed = (
        P(GROUPS_DP, None),
        P(GROUPS_DP),
        P(GROUPS_DP),
        P(GROUPS_DP, None),
        P(GROUPS_DP, None, "tp"),
        P("groups"),
        P(GROUPS_DP, "tp"),
        P(GROUPS_DP),
    )
    return jax.shard_map(
        functools.partial(shards, Z, X),
        mesh=torus,
        in_specs=placed,
        out_specs=(P(GROUPS_DP, None, "tp"), P(GROUPS_DP, "tp")),
        check_vma=False,
    )
```

```python
import functools
import math

import jax
import jax.numpy as jnp
from jax import lax
from jax.experimental import pallas as pl
from jax.experimental.pallas import tpu as pltpu
from jax.sharding import Mesh
from jax.sharding import PartitionSpec as P

LATENT_WIDTH = 512
ROTARY_WIDTH = 64
KEY = LATENT_WIDTH + ROTARY_WIDTH
PAIR = 2 * KEY
WIDE = LATENT_WIDTH + 2 * ROTARY_WIDTH
LANES = 128
TEAM_RANKS = 8
HEAD_BLOCK = 2
RIGHT_HOPS = (4, 3, 4, 3)
GROUPS_DP = ("groups", "dp_0", "dp_1")
MESH_ID = pl.DeviceIdType.MESH

log2_scale = 192.0 ** (-0.5) * math.log2(math.e)
masked_score = -1e30


def dot(a, b):
    return jnp.dot(a, b, preferred_element_type=jnp.float32)


def dot_t(a, b):
    return lax.dot_general(a, b, (((1,), (1,)), ((), ())), preferred_element_type=jnp.float32)


def iota(shape, dim):
    return lax.broadcasted_iota(jnp.int32, shape, dim)


def both_forms(low, high):
    low_lane = iota(low.shape, 1)
    low = jnp.where(low_lane < KEY, low.astype(jnp.float32), 0.0)
    high = jnp.where(low_lane >= ROTARY_WIDTH, high.astype(jnp.float32), 0.0)
    low_moved = pltpu.roll(low, ROTARY_WIDTH, 1)
    high_moved = pltpu.roll(high, WIDE - ROTARY_WIDTH, 1)
    cast = lambda a: a.astype(jnp.bfloat16)
    return cast(low), cast(low_moved), cast(high_moved), cast(high)


def finish(acc_first, acc_second, denominator):
    moved = pltpu.roll(acc_second, WIDE - ROTARY_WIDTH, 1)
    return (acc_first + moved[:, :LATENT_WIDTH]) / denominator


def kernel(
    Z,
    X,
    pool_hbm,
    q_hbm,
    dq_hbm,
    holder_ref,
    slot_ref,
    suffix_ref,
    len_ref,
    dlen_ref,
    out_ref,
    dout_ref,
    pool_ref,
    q_ref,
    dq_ref,
    c_ref,
    t_ref,
    w_ref,
    suf_ref,
    sendz,
    recvz,
    sendx,
    recvx,
    keys,
    q_first,
    q_second,
    peak_ref,
    total_ref,
    acc_first,
    acc_second,
    load_sem,
    c_send,
    c_recv,
    w_send,
    w_recv,
    s_send,
    s_recv,
    z_send,
    z_recv,
    x_send,
    x_recv,
    r_send,
    r_recv,
    l_send,
    l_recv,
    d_send,
    d_recv,
):
    my_z = lax.axis_index("dp_0")
    my_x = lax.axis_index("dp_1")
    my_c = lax.axis_index("tp")
    half = pool_ref.shape[1] // 2
    pages = pool_ref.shape[0]
    pull = keys.shape[2]
    zs = list(range(1, Z))
    xs = list(range(1, X))
    spans = []
    for at in range(0, half, PAIR):
        spans += [(at, at + LATENT_WIDTH), (at + LATENT_WIDTH, at + PAIR)]

    def at_z(d):
        return {"dp_0": lax.rem(my_z + d + Z, Z)}

    def at_x(e):
        return {"dp_1": lax.rem(my_x + e + X, X)}

    sibling = {"tp": 1 - my_c}

    def remote(src, dst, send, recv, where):
        return pltpu.make_async_remote_copy(
            src_ref=src, dst_ref=dst, send_sem=send, recv_sem=recv, device_id=where, device_id_type=MESH_ID
        )

    barrier = pltpu.get_barrier_semaphore()
    for d in zs:
        pl.semaphore_signal(barrier, inc=1, device_id=at_z(d), device_id_type=MESH_ID)
    for e in xs:
        pl.semaphore_signal(barrier, inc=1, device_id=at_x(e), device_id_type=MESH_ID)
    pl.semaphore_signal(barrier, inc=1, device_id=sibling, device_id_type=MESH_ID)
    loads = [
        pltpu.make_async_copy(src, dst, load_sem.at[n])
        for n, (src, dst) in enumerate([(pool_hbm, pool_ref), (q_hbm, q_ref), (dq_hbm, dq_ref)])
    ]
    for load in loads:
        load.start()

    holder = holder_ref[...]
    steps_z = lax.rem(my_z - holder // X + Z, Z)
    steps_x = lax.rem(my_x - holder % X + X, X)
    spots = (iota((LANES, pull), 0) == steps_x * Z + steps_z).astype(jnp.bfloat16)
    slot = jnp.broadcast_to((slot_ref[...] + 1).astype(jnp.float32), (8, pull)).astype(jnp.bfloat16)
    request = dot_t(slot, spots)
    c_ref[0] = request[:1]
    share = suf_ref.shape[1]
    flat = suffix_ref[...].astype(jnp.float32)
    suf_ref[0] = jnp.concatenate([flat[:, r * PAIR : (r + 1) * PAIR] for r in range(share)], axis=0).astype(
        jnp.bfloat16
    )
    pl.semaphore_wait(barrier, len(zs) + len(xs) + 1)

    c_copies = [remote(c_ref.at[0], c_ref.at[e], c_send.at[e], c_recv.at[e], at_x(-e)) for e in xs]
    for copy in c_copies:
        copy.start()
    s_copies = [remote(suf_ref.at[0], suf_ref.at[e], s_send.at[e], s_recv.at[e], at_x(e)) for e in xs]
    for copy in s_copies:
        copy.start()
    live = (request > 0.0).astype(jnp.bfloat16)
    before = (iota((LANES, LANES), 0) < iota((LANES, LANES), 1)).astype(jnp.bfloat16)
    place = dot(live, before)[:1].astype(jnp.int32)
    select = ((iota((pull, LANES), 0) == place) & (request[:1] > 0.0)).astype(jnp.bfloat16)
    loads[1].wait()
    prepare_queries(q_ref, q_first, q_second)
    for copy in c_copies:
        copy.wait_recv()
    rows = [c_ref[e] for e in range(X)]
    c_all = jnp.concatenate(rows + [jnp.zeros((LANES - X, LANES), jnp.float32)], axis=0)
    c_mine = jnp.where(iota((LANES, LANES), 1) // Z == iota((LANES, LANES), 0), c_all, 0.0).astype(jnp.bfloat16)
    pick = (iota((Z, LANES), 1) % Z == iota((Z, LANES), 0)).astype(jnp.bfloat16)
    table = dot_t(pick, c_mine)
    for d in range(Z):
        t_ref[d] = table[d : d + 1, :]

    w_copies = [remote(t_ref.at[d], w_ref.at[d], w_send.at[d], w_recv.at[d], at_z(-d)) for d in zs]
    for copy in w_copies:
        copy.start()
    w_ref[0] = t_ref[0]
    loads[0].wait()
    loads[2].wait()
    decode_rows(dlen_ref, dq_ref, pool_ref, dout_ref)
    for copy in w_copies:
        copy.wait_recv()
    spread = jnp.concatenate([jnp.broadcast_to(w_ref[d], (X, LANES)) for d in range(Z)], axis=0)
    mine = iota((Z * X, LANES), 1) == iota((Z * X, LANES), 0) % X
    wanted = jnp.sum(jnp.where(mine, spread, 0.0), axis=1, keepdims=True).astype(jnp.int32)
    gather = (wanted == iota((Z * X, pages), 1) + 1).astype(jnp.bfloat16)

    def along_z(k):
        lo, hi = spans[k]
        return [
            remote(sendz.at[d, :, lo:hi], recvz.at[d, :, lo:hi], z_send.at[k, d], z_recv.at[k, d], at_z(d)) for d in zs
        ]

    def along_x(k):
        lo, hi = spans[k]
        return [
            remote(sendx.at[e, :, lo:hi], recvx.at[e, :, lo:hi], x_send.at[k, e], x_recv.at[k, e], at_x(e)) for e in xs
        ]

    for k, (lo, hi) in enumerate(spans):
        start = pl.multiple_of(my_c * half + lo, LANES)
        taken = dot(gather, pool_ref[:, pl.ds(start, hi - lo)])
        sendz[:, :, lo:hi] = taken.reshape(Z, X, hi - lo).astype(jnp.bfloat16)
        for copy in along_z(k):
            copy.start()
        recvz[0, :, lo:hi] = sendz[0, :, lo:hi]

    of, to = iota((X * Z, Z * X), 1), iota((X * Z, Z * X), 0)
    turn = ((of % X == to // Z) & (of // X == to % Z)).astype(jnp.bfloat16)

    def pass_on(k):
        lo, hi = spans[k]
        for copy in along_z(k):
            copy.wait_recv()
        arrived = recvz[:, :, lo:hi].astype(jnp.float32).reshape(Z * X, hi - lo).astype(jnp.bfloat16)
        sendx[:, :, lo:hi] = dot(turn, arrived).reshape(X, Z, hi - lo).astype(jnp.bfloat16)
        for copy in along_x(k):
            copy.start()
        recvx[0, :, lo:hi] = sendx[0, :, lo:hi]

    def ring(k):
        lo, hi = spans[k]
        right_hops = RIGHT_HOPS[k % 4]
        left_hops = X - 1 - right_hops
        at = lambda side, s: keys.at[side, s, :, lo:hi]

        def to_right(i):
            return remote(at(0, i - 1), at(0, i), r_send.at[k, i], r_recv.at[k, i], at_x(1))

        def to_left(i):
            return remote(at(0, (X - i + 1) % X), at(0, X - i), l_send.at[k, i], l_recv.at[k, i], at_x(-1))

        def across(s):
            return remote(at(0, s), at(1, s), d_send.at[k, s], d_recv.at[k, s], sibling)

        def begin():
            for copy in along_x(k):
                copy.wait_recv()
            arrived = recvx[:, :, lo:hi].astype(jnp.float32).reshape(X * Z, hi - lo).astype(jnp.bfloat16)
            keys[0, 0, :, lo:hi] = dot(select[:, : X * Z], arrived).astype(jnp.bfloat16)
            if right_hops:
                to_right(1).start()
            if left_hops:
                to_left(1).start()
            across(0).start()

        def hop(i):
            if i <= right_hops:
                to_right(i).wait_recv()
                if i < right_hops:
                    to_right(i + 1).start()
                across(i).start()
            if i <= left_hops:
                to_left(i).wait_recv()
                if i < left_hops:
                    to_left(i + 1).start()
                across(X - i).start()

        def arrived():
            for s in range(X):
                across(s).wait_recv()

        def end():
            for i in range(1, right_hops + 1):
                to_right(i).wait_send()
            for i in range(1, left_hops + 1):
                to_left(i).wait_send()
            for s in range(X):
                across(s).wait_send()

        return begin, hop, arrived, end, max(right_hops, left_hops)

    rings = [ring(k) for k in range(len(spans))]
    length = len_ref[my_z]
    attend = functools.partial(
        attend_pair, X, my_x, length, keys, suf_ref, q_first, q_second, peak_ref, total_ref, acc_first, acc_second, out_ref
    )
    blocks = q_first.shape[0] // HEAD_BLOCK
    n_spans, hops = len(spans), max(r[4] for r in rings)
    waiting, done_rings = [], 0
    pass_on(0)
    for tick in range(n_spans + hops):
        if tick + 1 < n_spans:
            pass_on(tick + 1)
        for k in range(n_spans):
            i = tick - k
            if i == 0:
                rings[k][0]()
            elif 1 <= i <= rings[k][4]:
                rings[k][1](i)
                if i == rings[k][4]:
                    done_rings += 1
                    if done_rings == 2:
                        for copy in s_copies:
                            copy.wait_recv()
                    if done_rings % 2 == 0:
                        waiting += [(done_rings // 2 - 1, b) for b in range(blocks)]
        if waiting:
            p, b = waiting.pop(0)
            if b == 0:
                rings[2 * p][2]()
                rings[2 * p + 1][2]()
            attend(p, b)
    for p, b in waiting:
        if b == 0:
            rings[2 * p][2]()
            rings[2 * p + 1][2]()
        attend(p, b)

    for copy in c_copies + w_copies + s_copies:
        copy.wait_send()
    for k in range(n_spans):
        for copy in along_z(k) + along_x(k):
            copy.wait_send()
        rings[k][3]()


def prepare_queries(q_ref, q_first, q_second):
    for hp in range(q_ref.shape[1] // PAIR):
        low = q_ref[:, hp * PAIR : hp * PAIR + WIDE]
        high = q_ref[:, hp * PAIR + LATENT_WIDTH : (hp + 1) * PAIR]
        first_low, second_low, first_high, second_high = both_forms(low, high)
        q_first[2 * hp] = first_low
        q_second[2 * hp] = second_low
        q_first[2 * hp + 1] = first_high
        q_second[2 * hp + 1] = second_high


def attend_pair(
    X, my_x, length, keys, suf_ref, q_first, q_second, peak_ref, total_ref, acc_first, acc_second, out_ref, p, b
):
    tokens = q_first.shape[1]
    rows = HEAD_BLOCK * tokens
    heads = slice(b * HEAD_BLOCK, (b + 1) * HEAD_BLOCK)
    queries = [q_first[heads].reshape(rows, WIDE), q_second[heads].reshape(rows, WIDE)]
    share = suf_ref.shape[1]
    last = p == keys.shape[3] // PAIR - 1
    pieces, places = [], []
    if p == 0:
        token = iota((rows, share * X), 0) % tokens
        lane = iota((rows, share * X), 1)
        rank = lax.rem(my_x - lane // share + X, X)
        for par in range(2):
            at = par * LATENT_WIDTH
            k = suf_ref[:, :, at : at + WIDE].astype(jnp.float32).reshape(X * share, WIDE).astype(jnp.bfloat16)
            s = dot_t(queries[par], k) * log2_scale
            pos = rank * (2 * share) + 2 * (lane % share) + par
            pieces.append(jnp.where((pos <= token) & (pos < length), s, masked_score))
            places.append(k)
    for side in range(2):
        for par in range(2):
            at = p * PAIR + par * LATENT_WIDTH
            k = keys[side, :, :, at : at + WIDE].reshape(-1, WIDE)
            pieces.append(dot_t(queries[par], k) * log2_scale)
            places.append(k)
    peak = functools.reduce(jnp.maximum, [jnp.max(s, axis=1, keepdims=True) for s in pieces])
    if p:
        old = peak_ref[b][:, :1]
        peak = jnp.maximum(peak, old)
        factor = jnp.exp2(old - peak)
        total = total_ref[b][:, :1] * factor
        acc = [acc_first[b] * factor, acc_second[b] * factor]
    else:
        total = jnp.zeros((rows, 1), jnp.float32)
        acc = [jnp.zeros((rows, LATENT_WIDTH), jnp.float32), jnp.zeros((rows, WIDE), jnp.float32)]
    for n, s in enumerate(pieces):
        par = n % 2
        powers = jnp.exp2(s - peak)
        total = total + jnp.sum(powers, axis=1, keepdims=True)
        acc[par] = acc[par] + dot(powers.astype(jnp.bfloat16), places[n][:, : LATENT_WIDTH if par == 0 else WIDE])
    if not last:
        peak_ref[b] = jnp.broadcast_to(peak, (rows, LANES))
        total_ref[b] = jnp.broadcast_to(total, (rows, LANES))
        acc_first[b] = acc[0]
        acc_second[b] = acc[1]
        return
    result = finish(acc[0], acc[1], total)
    token = iota(result.shape, 0) % tokens
    result = jnp.where(token < length, result, 0.0).astype(jnp.bfloat16)
    for h in range(HEAD_BLOCK):
        at = (b * HEAD_BLOCK + h) * LATENT_WIDTH
        out_ref[:, at : at + LATENT_WIDTH] = result[h * tokens : (h + 1) * tokens]


def decode_rows(len_ref, dq_ref, pool_ref, out_ref):
    n_rows = dq_ref.shape[0]
    pages = pool_ref.shape[0]
    row_pages = pages // n_rows
    head_pairs = dq_ref.shape[1] // PAIR
    half = n_rows * head_pairs
    flat = dq_ref[...].astype(jnp.float32)
    queries = jnp.concatenate([flat[:, n * PAIR : (n + 1) * PAIR] for n in range(head_pairs)], axis=0)
    first_low, second_low, first_high, second_high = both_forms(queries[:, :WIDE], queries[:, LATENT_WIDTH:])
    queries = [
        jnp.concatenate([first_low, first_high], axis=0),
        jnp.concatenate([second_low, second_high], axis=0),
    ]
    count = 2 * half
    page = iota((count, pages), 1)
    owner = iota((count, pages), 0) % n_rows
    limit = jnp.zeros((count, pages), jnp.int32)
    for r in range(n_rows):
        limit = jnp.where(owner == r, len_ref[r], limit)
    limit = jnp.where(page // row_pages == owner, limit, 0)
    page_tokens = pool_ref.shape[1] // KEY
    pieces = []
    for n in range(page_tokens):
        at = (n // 2) * PAIR + (n % 2) * LATENT_WIDTH
        s = dot_t(queries[n % 2], pool_ref[:, at : at + WIDE]) * log2_scale
        pieces.append(jnp.where((page % row_pages) * page_tokens + n < limit, s, masked_score))
    peak = functools.reduce(jnp.maximum, [jnp.max(s, axis=1, keepdims=True) for s in pieces])
    total = jnp.zeros((count, 1), jnp.float32)
    acc = [jnp.zeros((count, LATENT_WIDTH), jnp.float32), jnp.zeros((count, WIDE), jnp.float32)]
    for n in range(page_tokens):
        at = (n // 2) * PAIR + (n % 2) * LATENT_WIDTH
        width = LATENT_WIDTH if n % 2 == 0 else WIDE
        powers = jnp.exp2(pieces[n] - peak)
        total = total + jnp.sum(powers, axis=1, keepdims=True)
        acc[n % 2] = acc[n % 2] + dot(powers.astype(jnp.bfloat16), pool_ref[:, at : at + width])
    result = finish(acc[0], acc[1], total).astype(jnp.float32)
    for n in range(head_pairs):
        at = n * 2 * LATENT_WIDTH
        low = slice(n * n_rows, (n + 1) * n_rows)
        high = slice(half + n * n_rows, half + (n + 1) * n_rows)
        out_ref[:, at : at + LATENT_WIDTH] = result[low].astype(jnp.bfloat16)
        out_ref[:, at + LATENT_WIDTH : at + 2 * LATENT_WIDTH] = result[high].astype(jnp.bfloat16)


def shards(
    Z,
    X,
    pool,
    page_holder,
    page_slot,
    suffix_latent_rows,
    prefill_queries,
    suffix_len,
    decode_queries,
    decode_len,
):
    pages = pool.shape[0]
    pull = page_holder.shape[0]
    half = pool.shape[1] // 2
    tokens = prefill_queries.shape[1]
    heads = prefill_queries.shape[2] // KEY
    decode_heads = decode_queries.shape[1] // KEY
    share = suffix_latent_rows.shape[1] // PAIR
    n_spans = 2 * half // PAIR
    blocks = heads // HEAD_BLOCK
    rows = HEAD_BLOCK * tokens
    bf16, f32 = jnp.bfloat16, jnp.float32
    hbm, vmem, smem = (pl.BlockSpec(memory_space=m) for m in (pl.ANY, pltpu.VMEM, pltpu.SMEM))
    dma = pltpu.SemaphoreType.DMA
    prefill_part, decode_part = pl.pallas_call(
        functools.partial(kernel, Z, X),
        out_shape=(
            jax.ShapeDtypeStruct((tokens, heads * LATENT_WIDTH), bf16),
            jax.ShapeDtypeStruct((decode_queries.shape[0], decode_heads * LATENT_WIDTH), bf16),
        ),
        in_specs=[hbm, hbm, hbm, vmem, vmem, vmem, smem, smem],
        out_specs=(vmem, vmem),
        scratch_shapes=[
            pltpu.VMEM(pool.shape, bf16),
            pltpu.VMEM((tokens, heads * KEY), bf16),
            pltpu.VMEM(decode_queries.shape, bf16),
            pltpu.VMEM((X, 1, LANES), f32),
            pltpu.VMEM((Z, 1, LANES), f32),
            pltpu.VMEM((Z, 1, LANES), f32),
            pltpu.VMEM((X, share, PAIR), bf16),
            pltpu.VMEM((Z, X, half), bf16),
            pltpu.VMEM((Z, X, half), bf16),
            pltpu.VMEM((X, Z, half), bf16),
            pltpu.VMEM((X, Z, half), bf16),
            pltpu.VMEM((2, X, pull, half), bf16),
            pltpu.VMEM((heads, tokens, WIDE), bf16),
            pltpu.VMEM((heads, tokens, WIDE), bf16),
            pltpu.VMEM((blocks, rows, LANES), f32),
            pltpu.VMEM((blocks, rows, LANES), f32),
            pltpu.VMEM((blocks, rows, LATENT_WIDTH), f32),
            pltpu.VMEM((blocks, rows, WIDE), f32),
            dma((3,)),
            dma((X,)),
            dma((X,)),
            dma((Z,)),
            dma((Z,)),
            dma((X,)),
            dma((X,)),
            dma((n_spans, Z)),
            dma((n_spans, Z)),
            dma((n_spans, X)),
            dma((n_spans, X)),
            dma((n_spans, X)),
            dma((n_spans, X)),
            dma((n_spans, X)),
            dma((n_spans, X)),
            dma((n_spans, X)),
            dma((n_spans, X)),
        ],
        compiler_params=pltpu.CompilerParams(
            collective_id=0, has_side_effects=True, vmem_limit_bytes=60 * 1024 * 1024
        ),
        name="whole",
    )(
        pool,
        prefill_queries[0],
        decode_queries,
        page_holder[None],
        page_slot[None],
        suffix_latent_rows,
        suffix_len,
        decode_len,
    )
    return (prefill_part[None], decode_part)


def solution(mesh):
    groups, dp, tp = (mesh.shape[name] for name in ("groups", "dp", "tp"))
    X = TEAM_RANKS
    Z = dp // X
    torus = Mesh(mesh.devices.reshape(groups, Z, X, tp), ("groups", "dp_0", "dp_1", "tp"))
    placed = (
        P(GROUPS_DP, None),
        P(GROUPS_DP),
        P(GROUPS_DP),
        P(GROUPS_DP, None),
        P(GROUPS_DP, None, "tp"),
        P("groups"),
        P(GROUPS_DP, "tp"),
        P(GROUPS_DP),
    )
    return jax.shard_map(
        functools.partial(shards, Z, X),
        mesh=torus,
        in_specs=placed,
        out_specs=(P(GROUPS_DP, None, "tp"), P(GROUPS_DP, "tp")),
        check_vma=False,
    )
```

```python
import functools
import math

import jax
import jax.numpy as jnp
from jax import lax
from jax.experimental import pallas as pl
from jax.experimental.pallas import tpu as pltpu
from jax.sharding import Mesh
from jax.sharding import PartitionSpec as P

LATENT_WIDTH = 512
ROTARY_WIDTH = 64
KEY = LATENT_WIDTH + ROTARY_WIDTH
PAIR = 2 * KEY
WIDE = LATENT_WIDTH + 2 * ROTARY_WIDTH
LANES = 128
TEAM_RANKS = 8
HEAD_BLOCK = 2
RIGHT_HOPS = (4, 3, 4, 3)
ROUTES = ("zx", "zx", "xz", "xz")
STEPS = (
    "s0", "s2", "s1", "s3", "p2", "p3", "p0", "p1", "b0", "b1", "h01", "h11",
    "b2", "h02", "h12", "h21", "b3", "h03", "h13", "h22", "h31", "h04", "h14", "h23",
    "h32", "w0", "w1", "a00", "h24", "h33", "a01", "h34", "w2", "w3", "a10", "a11",
)
GROUPS_DP = ("groups", "dp_0", "dp_1")
MESH_ID = pl.DeviceIdType.MESH

log2_scale = 192.0 ** (-0.5) * math.log2(math.e)
masked_score = -1e30


def dot(a, b):
    return jnp.dot(a, b, preferred_element_type=jnp.float32)


def dot_t(a, b):
    return lax.dot_general(a, b, (((1,), (1,)), ((), ())), preferred_element_type=jnp.float32)


def iota(shape, dim):
    return lax.broadcasted_iota(jnp.int32, shape, dim)


def both_forms(low, high):
    low_lane = iota(low.shape, 1)
    low = jnp.where(low_lane < KEY, low.astype(jnp.float32), 0.0)
    high = jnp.where(low_lane >= ROTARY_WIDTH, high.astype(jnp.float32), 0.0)
    low_moved = pltpu.roll(low, ROTARY_WIDTH, 1)
    high_moved = pltpu.roll(high, WIDE - ROTARY_WIDTH, 1)
    cast = lambda a: a.astype(jnp.bfloat16)
    return cast(low), cast(low_moved), cast(high_moved), cast(high)


def finish(acc_first, acc_second, denominator):
    moved = pltpu.roll(acc_second, WIDE - ROTARY_WIDTH, 1)
    return (acc_first + moved[:, :LATENT_WIDTH]) / denominator


def kernel(
    Z,
    X,
    pool_hbm,
    q_hbm,
    dq_hbm,
    holder_ref,
    slot_ref,
    suffix_ref,
    len_ref,
    dlen_ref,
    out_ref,
    dout_ref,
    pool_ref,
    q_ref,
    dq_ref,
    c_ref,
    t_ref,
    w_ref,
    suf_ref,
    sendz,
    recvz,
    sendx,
    recvx,
    keys,
    q_first,
    q_second,
    peak_ref,
    total_ref,
    acc_first,
    acc_second,
    load_sem,
    c_send,
    c_recv,
    w_send,
    w_recv,
    s_send,
    s_recv,
    z_send,
    z_recv,
    x_send,
    x_recv,
    r_send,
    r_recv,
    l_send,
    l_recv,
    d_send,
    d_recv,
):
    my_z = lax.axis_index("dp_0")
    my_x = lax.axis_index("dp_1")
    my_c = lax.axis_index("tp")
    half = pool_ref.shape[1] // 2
    pages = pool_ref.shape[0]
    pull = keys.shape[2]
    zs = list(range(1, Z))
    xs = list(range(1, X))
    spans = []
    for at in range(0, half, PAIR):
        spans += [(at, at + LATENT_WIDTH), (at + LATENT_WIDTH, at + PAIR)]

    def at_z(d):
        return {"dp_0": lax.rem(my_z + d + Z, Z)}

    def at_x(e):
        return {"dp_1": lax.rem(my_x + e + X, X)}

    sibling = {"tp": 1 - my_c}

    def remote(src, dst, send, recv, where):
        return pltpu.make_async_remote_copy(
            src_ref=src, dst_ref=dst, send_sem=send, recv_sem=recv, device_id=where, device_id_type=MESH_ID
        )

    barrier = pltpu.get_barrier_semaphore()
    for d in zs:
        pl.semaphore_signal(barrier, inc=1, device_id=at_z(d), device_id_type=MESH_ID)
    for e in xs:
        pl.semaphore_signal(barrier, inc=1, device_id=at_x(e), device_id_type=MESH_ID)
    pl.semaphore_signal(barrier, inc=1, device_id=sibling, device_id_type=MESH_ID)
    loads = [
        pltpu.make_async_copy(src, dst, load_sem.at[n])
        for n, (src, dst) in enumerate([(pool_hbm, pool_ref), (q_hbm, q_ref), (dq_hbm, dq_ref)])
    ]
    for load in loads:
        load.start()

    holder = holder_ref[...]
    steps_z = lax.rem(my_z - holder // X + Z, Z)
    steps_x = lax.rem(my_x - holder % X + X, X)
    spots = (iota((LANES, pull), 0) == steps_x * Z + steps_z).astype(jnp.bfloat16)
    slot = jnp.broadcast_to((slot_ref[...] + 1).astype(jnp.float32), (8, pull)).astype(jnp.bfloat16)
    request = dot_t(slot, spots)
    c_ref[0] = request[:1]
    share = suf_ref.shape[1]
    flat = suffix_ref[...].astype(jnp.float32)
    suf_ref[0] = jnp.concatenate([flat[:, r * PAIR : (r + 1) * PAIR] for r in range(share)], axis=0).astype(
        jnp.bfloat16
    )
    pl.semaphore_wait(barrier, len(zs) + len(xs) + 1)

    c_copies = [remote(c_ref.at[0], c_ref.at[e], c_send.at[e], c_recv.at[e], at_x(-e)) for e in xs]
    for copy in c_copies:
        copy.start()
    s_copies = [remote(suf_ref.at[0], suf_ref.at[e], s_send.at[e], s_recv.at[e], at_x(e)) for e in xs]
    for copy in s_copies:
        copy.start()
    live = (request > 0.0).astype(jnp.bfloat16)
    before = (iota((LANES, LANES), 0) < iota((LANES, LANES), 1)).astype(jnp.bfloat16)
    place = dot(live, before)[:1].astype(jnp.int32)
    select = ((iota((pull, LANES), 0) == place) & (request[:1] > 0.0)).astype(jnp.bfloat16)
    loads[1].wait()
    prepare_queries(q_ref, q_first, q_second)
    for copy in c_copies:
        copy.wait_recv()
    rows = [c_ref[e] for e in range(X)]
    c_all = jnp.concatenate(rows + [jnp.zeros((LANES - X, LANES), jnp.float32)], axis=0)
    c_mine = jnp.where(iota((LANES, LANES), 1) // Z == iota((LANES, LANES), 0), c_all, 0.0).astype(jnp.bfloat16)
    pick = (iota((Z, LANES), 1) % Z == iota((Z, LANES), 0)).astype(jnp.bfloat16)
    table = dot_t(pick, c_mine)
    for d in range(Z):
        t_ref[d] = table[d : d + 1, :]

    w_copies = [remote(t_ref.at[d], w_ref.at[d], w_send.at[d], w_recv.at[d], at_z(-d)) for d in zs]
    for copy in w_copies:
        copy.start()
    w_ref[0] = t_ref[0]
    loads[0].wait()
    loads[2].wait()
    decode_rows(dlen_ref, dq_ref, pool_ref, dout_ref)
    for copy in w_copies:
        copy.wait_recv()
    spread = jnp.concatenate([jnp.broadcast_to(w_ref[d], (X, LANES)) for d in range(Z)], axis=0)
    mine = iota((Z * X, LANES), 1) == iota((Z * X, LANES), 0) % X
    wanted = jnp.sum(jnp.where(mine, spread, 0.0), axis=1, keepdims=True).astype(jnp.int32)
    gather = (wanted == iota((Z * X, pages), 1) + 1).astype(jnp.bfloat16)

    def along_z(k):
        lo, hi = spans[k]
        return [
            remote(sendz.at[d, :, lo:hi], recvz.at[d, :, lo:hi], z_send.at[k, d], z_recv.at[k, d], at_z(d)) for d in zs
        ]

    def along_x(k):
        lo, hi = spans[k]
        return [
            remote(sendx.at[e, :, lo:hi], recvx.at[e, :, lo:hi], x_send.at[k, e], x_recv.at[k, e], at_x(e)) for e in xs
        ]

    of, to = iota((X * Z, Z * X), 1), iota((X * Z, Z * X), 0)
    turn = ((of % X == to // Z) & (of // X == to % Z)).astype(jnp.bfloat16)
    back = ((of % Z == to // X) & (of // Z == to % X)).astype(jnp.bfloat16)
    orders = {"zx": (gather, select[:, : X * Z]), "xz": (None, None)}
    orders["xz"] = tuple(
        m.astype(jnp.bfloat16) for m in (dot(turn, gather), dot(select[:, : X * Z], turn))
    )

    def put_z(k, rows):
        lo, hi = spans[k]
        sendz[:, :, lo:hi] = rows.reshape(Z, X, hi - lo).astype(jnp.bfloat16)
        for copy in along_z(k):
            copy.start()
        recvz[0, :, lo:hi] = sendz[0, :, lo:hi]

    def put_x(k, rows):
        lo, hi = spans[k]
        sendx[:, :, lo:hi] = rows.reshape(X, Z, hi - lo).astype(jnp.bfloat16)
        for copy in along_x(k):
            copy.start()
        recvx[0, :, lo:hi] = sendx[0, :, lo:hi]

    def got(k, axis):
        lo, hi = spans[k]
        for copy in along_z(k) if axis == "z" else along_x(k):
            copy.wait_recv()
        ref = recvz if axis == "z" else recvx
        return ref[:, :, lo:hi].astype(jnp.float32).reshape(X * Z, hi - lo).astype(jnp.bfloat16)

    def send(k):
        lo, hi = spans[k]
        start = pl.multiple_of(my_c * half + lo, LANES)
        taken = dot(orders[ROUTES[k]][0], pool_ref[:, pl.ds(start, hi - lo)])
        (put_z if ROUTES[k] == "zx" else put_x)(k, taken)

    def pass_on(k):
        if ROUTES[k] == "zx":
            put_x(k, dot(turn, got(k, "z")))
        else:
            put_z(k, dot(back, got(k, "x")))

    def ring(k):
        lo, hi = spans[k]
        right_hops = RIGHT_HOPS[k % 4]
        left_hops = X - 1 - right_hops
        at = lambda side, s: keys.at[side, s, :, lo:hi]

        def to_right(i):
            return remote(at(0, i - 1), at(0, i), r_send.at[k, i], r_recv.at[k, i], at_x(1))

        def to_left(i):
            return remote(at(0, (X - i + 1) % X), at(0, X - i), l_send.at[k, i], l_recv.at[k, i], at_x(-1))

        def across(s):
            return remote(at(0, s), at(1, s), d_send.at[k, s], d_recv.at[k, s], sibling)

        def begin():
            keys[0, 0, :, lo:hi] = dot(orders[ROUTES[k]][1], got(k, ROUTES[k][1])).astype(jnp.bfloat16)
            if right_hops:
                to_right(1).start()
            if left_hops:
                to_left(1).start()
            across(0).start()

        def hop(i):
            if i <= right_hops:
                to_right(i).wait_recv()
                if i < right_hops:
                    to_right(i + 1).start()
                across(i).start()
            if i <= left_hops:
                to_left(i).wait_recv()
                if i < left_hops:
                    to_left(i + 1).start()
                across(X - i).start()

        def arrived():
            for s in range(X):
                across(s).wait_recv()

        def end():
            for i in range(1, right_hops + 1):
                to_right(i).wait_send()
            for i in range(1, left_hops + 1):
                to_left(i).wait_send()
            for s in range(X):
                across(s).wait_send()

        return begin, hop, arrived, end, max(right_hops, left_hops)

    rings = [ring(k) for k in range(len(spans))]
    length = len_ref[my_z]
    attend = functools.partial(
        attend_pair, X, my_x, length, keys, suf_ref, q_first, q_second, peak_ref, total_ref, acc_first, acc_second, out_ref
    )
    blocks = q_first.shape[0] // HEAD_BLOCK
    n_spans = len(spans)
    for copy in s_copies:
        copy.wait_recv()
    for step in STEPS:
        what, numbers = step[0], [int(n) for n in step[1:]]
        if what == "s":
            send(*numbers)
        elif what == "p":
            pass_on(*numbers)
        elif what == "b":
            rings[numbers[0]][0]()
        elif what == "h":
            k, i = numbers
            if i <= rings[k][4]:
                rings[k][1](i)
        elif what == "w":
            rings[numbers[0]][2]()
        elif what == "a":
            attend(*numbers)

    for copy in c_copies + w_copies + s_copies:
        copy.wait_send()
    for k in range(n_spans):
        for copy in along_z(k) + along_x(k):
            copy.wait_send()
        rings[k][3]()


def prepare_queries(q_ref, q_first, q_second):
    for hp in range(q_ref.shape[1] // PAIR):
        low = q_ref[:, hp * PAIR : hp * PAIR + WIDE]
        high = q_ref[:, hp * PAIR + LATENT_WIDTH : (hp + 1) * PAIR]
        first_low, second_low, first_high, second_high = both_forms(low, high)
        q_first[2 * hp] = first_low
        q_second[2 * hp] = second_low
        q_first[2 * hp + 1] = first_high
        q_second[2 * hp + 1] = second_high


def attend_pair(
    X, my_x, length, keys, suf_ref, q_first, q_second, peak_ref, total_ref, acc_first, acc_second, out_ref, p, b
):
    tokens = q_first.shape[1]
    rows = HEAD_BLOCK * tokens
    heads = slice(b * HEAD_BLOCK, (b + 1) * HEAD_BLOCK)
    queries = [q_first[heads].reshape(rows, WIDE), q_second[heads].reshape(rows, WIDE)]
    share = suf_ref.shape[1]
    last = p == keys.shape[3] // PAIR - 1
    pieces, places = [], []
    if p == 0:
        token = iota((rows, share * X), 0) % tokens
        lane = iota((rows, share * X), 1)
        rank = lax.rem(my_x - lane // share + X, X)
        for par in range(2):
            at = par * LATENT_WIDTH
            k = suf_ref[:, :, at : at + WIDE].astype(jnp.float32).reshape(X * share, WIDE).astype(jnp.bfloat16)
            s = dot_t(queries[par], k) * log2_scale
            pos = rank * (2 * share) + 2 * (lane % share) + par
            pieces.append(jnp.where((pos <= token) & (pos < length), s, masked_score))
            places.append(k)
    for side in range(2):
        for par in range(2):
            at = p * PAIR + par * LATENT_WIDTH
            k = keys[side, :, :, at : at + WIDE].reshape(-1, WIDE)
            pieces.append(dot_t(queries[par], k) * log2_scale)
            places.append(k)
    peak = functools.reduce(jnp.maximum, [jnp.max(s, axis=1, keepdims=True) for s in pieces])
    if p:
        old = peak_ref[b][:, :1]
        peak = jnp.maximum(peak, old)
        factor = jnp.exp2(old - peak)
        total = total_ref[b][:, :1] * factor
        acc = [acc_first[b] * factor, acc_second[b] * factor]
    else:
        total = jnp.zeros((rows, 1), jnp.float32)
        acc = [jnp.zeros((rows, LATENT_WIDTH), jnp.float32), jnp.zeros((rows, WIDE), jnp.float32)]
    for n, s in enumerate(pieces):
        par = n % 2
        powers = jnp.exp2(s - peak)
        total = total + jnp.sum(powers, axis=1, keepdims=True)
        acc[par] = acc[par] + dot(powers.astype(jnp.bfloat16), places[n][:, : LATENT_WIDTH if par == 0 else WIDE])
    if not last:
        peak_ref[b] = jnp.broadcast_to(peak, (rows, LANES))
        total_ref[b] = jnp.broadcast_to(total, (rows, LANES))
        acc_first[b] = acc[0]
        acc_second[b] = acc[1]
        return
    result = finish(acc[0], acc[1], total)
    token = iota(result.shape, 0) % tokens
    result = jnp.where(token < length, result, 0.0).astype(jnp.bfloat16)
    for h in range(HEAD_BLOCK):
        at = (b * HEAD_BLOCK + h) * LATENT_WIDTH
        out_ref[:, at : at + LATENT_WIDTH] = result[h * tokens : (h + 1) * tokens]


def decode_rows(len_ref, dq_ref, pool_ref, out_ref):
    n_rows = dq_ref.shape[0]
    pages = pool_ref.shape[0]
    row_pages = pages // n_rows
    head_pairs = dq_ref.shape[1] // PAIR
    half = n_rows * head_pairs
    flat = dq_ref[...].astype(jnp.float32)
    queries = jnp.concatenate([flat[:, n * PAIR : (n + 1) * PAIR] for n in range(head_pairs)], axis=0)
    first_low, second_low, first_high, second_high = both_forms(queries[:, :WIDE], queries[:, LATENT_WIDTH:])
    queries = [
        jnp.concatenate([first_low, first_high], axis=0),
        jnp.concatenate([second_low, second_high], axis=0),
    ]
    count = 2 * half
    page = iota((count, pages), 1)
    owner = iota((count, pages), 0) % n_rows
    limit = jnp.zeros((count, pages), jnp.int32)
    for r in range(n_rows):
        limit = jnp.where(owner == r, len_ref[r], limit)
    limit = jnp.where(page // row_pages == owner, limit, 0)
    page_tokens = pool_ref.shape[1] // KEY
    pieces = []
    for n in range(page_tokens):
        at = (n // 2) * PAIR + (n % 2) * LATENT_WIDTH
        s = dot_t(queries[n % 2], pool_ref[:, at : at + WIDE]) * log2_scale
        pieces.append(jnp.where((page % row_pages) * page_tokens + n < limit, s, masked_score))
    peak = functools.reduce(jnp.maximum, [jnp.max(s, axis=1, keepdims=True) for s in pieces])
    total = jnp.zeros((count, 1), jnp.float32)
    acc = [jnp.zeros((count, LATENT_WIDTH), jnp.float32), jnp.zeros((count, WIDE), jnp.float32)]
    for n in range(page_tokens):
        at = (n // 2) * PAIR + (n % 2) * LATENT_WIDTH
        width = LATENT_WIDTH if n % 2 == 0 else WIDE
        powers = jnp.exp2(pieces[n] - peak)
        total = total + jnp.sum(powers, axis=1, keepdims=True)
        acc[n % 2] = acc[n % 2] + dot(powers.astype(jnp.bfloat16), pool_ref[:, at : at + width])
    result = finish(acc[0], acc[1], total).astype(jnp.float32)
    for n in range(head_pairs):
        at = n * 2 * LATENT_WIDTH
        low = slice(n * n_rows, (n + 1) * n_rows)
        high = slice(half + n * n_rows, half + (n + 1) * n_rows)
        out_ref[:, at : at + LATENT_WIDTH] = result[low].astype(jnp.bfloat16)
        out_ref[:, at + LATENT_WIDTH : at + 2 * LATENT_WIDTH] = result[high].astype(jnp.bfloat16)


def hand_over(a_in, b_in, a_out, b_out, a_held, b_held, in_sem, out_sem):
    takes = [pltpu.make_async_copy(a_in, a_held, in_sem.at[0]), pltpu.make_async_copy(b_in, b_held, in_sem.at[1])]
    gives = [pltpu.make_async_copy(a_held, a_out, out_sem.at[0]), pltpu.make_async_copy(b_held, b_out, out_sem.at[1])]
    for copy in takes:
        copy.start()
    for take, give in zip(takes, gives):
        take.wait()
        give.start()
    for copy in gives:
        copy.wait()


def shards(
    Z,
    X,
    pool,
    page_holder,
    page_slot,
    suffix_latent_rows,
    prefill_queries,
    suffix_len,
    decode_queries,
    decode_len,
):
    pages = pool.shape[0]
    pull = page_holder.shape[0]
    half = pool.shape[1] // 2
    tokens = prefill_queries.shape[1]
    heads = prefill_queries.shape[2] // KEY
    decode_heads = decode_queries.shape[1] // KEY
    share = suffix_latent_rows.shape[1] // PAIR
    n_spans = 2 * half // PAIR
    blocks = heads // HEAD_BLOCK
    rows = HEAD_BLOCK * tokens
    bf16, f32 = jnp.bfloat16, jnp.float32
    hbm, vmem, smem = (pl.BlockSpec(memory_space=m) for m in (pl.ANY, pltpu.VMEM, pltpu.SMEM))
    dma = pltpu.SemaphoreType.DMA
    prefill_part, decode_part = pl.pallas_call(
        functools.partial(kernel, Z, X),
        out_shape=(
            jax.ShapeDtypeStruct((tokens, heads * LATENT_WIDTH), bf16),
            jax.ShapeDtypeStruct((decode_queries.shape[0], decode_heads * LATENT_WIDTH), bf16),
        ),
        in_specs=[hbm, hbm, hbm, vmem, vmem, vmem, smem, smem],
        out_specs=(vmem, vmem),
        scratch_shapes=[
            pltpu.VMEM(pool.shape, bf16),
            pltpu.VMEM((tokens, heads * KEY), bf16),
            pltpu.VMEM(decode_queries.shape, bf16),
            pltpu.VMEM((X, 1, LANES), f32),
            pltpu.VMEM((Z, 1, LANES), f32),
            pltpu.VMEM((Z, 1, LANES), f32),
            pltpu.VMEM((X, share, PAIR), bf16),
            pltpu.VMEM((Z, X, half), bf16),
            pltpu.VMEM((Z, X, half), bf16),
            pltpu.VMEM((X, Z, half), bf16),
            pltpu.VMEM((X, Z, half), bf16),
            pltpu.VMEM((2, X, pull, half), bf16),
            pltpu.VMEM((heads, tokens, WIDE), bf16),
            pltpu.VMEM((heads, tokens, WIDE), bf16),
            pltpu.VMEM((blocks, rows, LANES), f32),
            pltpu.VMEM((blocks, rows, LANES), f32),
            pltpu.VMEM((blocks, rows, LATENT_WIDTH), f32),
            pltpu.VMEM((blocks, rows, WIDE), f32),
            dma((3,)),
            dma((X,)),
            dma((X,)),
            dma((Z,)),
            dma((Z,)),
            dma((X,)),
            dma((X,)),
            dma((n_spans, Z)),
            dma((n_spans, Z)),
            dma((n_spans, X)),
            dma((n_spans, X)),
            dma((n_spans, X)),
            dma((n_spans, X)),
            dma((n_spans, X)),
            dma((n_spans, X)),
            dma((n_spans, X)),
            dma((n_spans, X)),
        ],
        compiler_params=pltpu.CompilerParams(
            collective_id=0, has_side_effects=True, vmem_limit_bytes=60 * 1024 * 1024
        ),
        name="whole",
    )(
        pool,
        prefill_queries[0],
        decode_queries,
        page_holder[None],
        page_slot[None],
        suffix_latent_rows,
        suffix_len,
        decode_len,
    )
    prefill_part, decode_part = pl.pallas_call(
        hand_over,
        out_shape=tuple(jax.ShapeDtypeStruct(a.shape, a.dtype) for a in (prefill_part, decode_part)),
        in_specs=[hbm, hbm],
        out_specs=(hbm, hbm),
        scratch_shapes=[
            pltpu.VMEM(prefill_part.shape, bf16),
            pltpu.VMEM(decode_part.shape, bf16),
            dma((2,)),
            dma((2,)),
        ],
        compiler_params=pltpu.CompilerParams(vmem_limit_bytes=60 * 1024 * 1024),
        name="hand_over",
    )(prefill_part, decode_part)
    return (prefill_part[None], decode_part)


def solution(mesh):
    groups, dp, tp = (mesh.shape[name] for name in ("groups", "dp", "tp"))
    X = TEAM_RANKS
    Z = dp // X
    torus = Mesh(mesh.devices.reshape(groups, Z, X, tp), ("groups", "dp_0", "dp_1", "tp"))
    placed = (
        P(GROUPS_DP, None),
        P(GROUPS_DP),
        P(GROUPS_DP),
        P(GROUPS_DP, None),
        P(GROUPS_DP, None, "tp"),
        P("groups"),
        P(GROUPS_DP, "tp"),
        P(GROUPS_DP),
    )
    return jax.shard_map(
        functools.partial(shards, Z, X),
        mesh=torus,
        in_specs=placed,
        out_specs=(P(GROUPS_DP, None, "tp"), P(GROUPS_DP, "tp")),
        check_vma=False,
    )
```

```python
import functools
import math

import jax
import jax.numpy as jnp
from jax import lax
from jax.experimental import pallas as pl
from jax.experimental.pallas import tpu as pltpu
from jax.sharding import Mesh
from jax.sharding import PartitionSpec as P

LATENT_WIDTH = 512
ROTARY_WIDTH = 64
KEY = LATENT_WIDTH + ROTARY_WIDTH
PAIR = 2 * KEY
WIDE = LATENT_WIDTH + 2 * ROTARY_WIDTH
LANES = 128
TEAM_RANKS = 8
HEAD_BLOCK = 2
RIGHT_HOPS = (4, 3, 4, 3)
ROUTES = ("zx", "xz", "xz", "xz")
STEPS = (
    "s0", "s1", "s2", "s3", "p1", "p2", "p3", "p0", "b0", "b1", "h01", "h11",
    "b2", "h02", "h12", "h21", "b3", "h03", "h13", "h22", "h31", "h04", "h14", "h23",
    "h32", "h24", "h33", "w0", "w1", "a00", "a01", "h34", "w2", "w3", "a10", "a11",
)
GROUPS_DP = ("groups", "dp_0", "dp_1")
MESH_ID = pl.DeviceIdType.MESH

log2_scale = 192.0 ** (-0.5) * math.log2(math.e)
masked_score = -1e30


def dot(a, b):
    return jnp.dot(a, b, preferred_element_type=jnp.float32)


def dot_t(a, b):
    return lax.dot_general(a, b, (((1,), (1,)), ((), ())), preferred_element_type=jnp.float32)


def iota(shape, dim):
    return lax.broadcasted_iota(jnp.int32, shape, dim)


def both_forms(low, high):
    low_lane = iota(low.shape, 1)
    low = jnp.where(low_lane < KEY, low.astype(jnp.float32), 0.0)
    high = jnp.where(low_lane >= ROTARY_WIDTH, high.astype(jnp.float32), 0.0)
    low_moved = pltpu.roll(low, ROTARY_WIDTH, 1)
    high_moved = pltpu.roll(high, WIDE - ROTARY_WIDTH, 1)
    cast = lambda a: a.astype(jnp.bfloat16)
    return cast(low), cast(low_moved), cast(high_moved), cast(high)


def finish(acc_first, acc_second, denominator):
    moved = pltpu.roll(acc_second, WIDE - ROTARY_WIDTH, 1)
    return (acc_first + moved[:, :LATENT_WIDTH]) / denominator


def kernel(
    Z,
    X,
    pool_hbm,
    q_hbm,
    dq_hbm,
    holder_ref,
    slot_ref,
    suffix_ref,
    len_ref,
    dlen_ref,
    out_ref,
    dout_ref,
    pool_ref,
    q_ref,
    dq_ref,
    c_ref,
    t_ref,
    w_ref,
    suf_ref,
    sendz,
    recvz,
    sendx,
    recvx,
    keys,
    q_first,
    q_second,
    peak_ref,
    total_ref,
    acc_first,
    acc_second,
    load_sem,
    c_send,
    c_recv,
    w_send,
    w_recv,
    s_send,
    s_recv,
    z_send,
    z_recv,
    x_send,
    x_recv,
    r_send,
    r_recv,
    l_send,
    l_recv,
    d_send,
    d_recv,
):
    my_z = lax.axis_index("dp_0")
    my_x = lax.axis_index("dp_1")
    my_c = lax.axis_index("tp")
    half = pool_ref.shape[1] // 2
    pages = pool_ref.shape[0]
    pull = keys.shape[2]
    zs = list(range(1, Z))
    xs = list(range(1, X))
    spans = []
    for at in range(0, half, PAIR):
        spans += [(at, at + LATENT_WIDTH), (at + LATENT_WIDTH, at + PAIR)]

    def at_z(d):
        return {"dp_0": lax.rem(my_z + d + Z, Z)}

    def at_x(e):
        return {"dp_1": lax.rem(my_x + e + X, X)}

    sibling = {"tp": 1 - my_c}

    def remote(src, dst, send, recv, where):
        return pltpu.make_async_remote_copy(
            src_ref=src, dst_ref=dst, send_sem=send, recv_sem=recv, device_id=where, device_id_type=MESH_ID
        )

    barrier = pltpu.get_barrier_semaphore()
    for d in zs:
        pl.semaphore_signal(barrier, inc=1, device_id=at_z(d), device_id_type=MESH_ID)
    for e in xs:
        pl.semaphore_signal(barrier, inc=1, device_id=at_x(e), device_id_type=MESH_ID)
    pl.semaphore_signal(barrier, inc=1, device_id=sibling, device_id_type=MESH_ID)
    loads = [
        pltpu.make_async_copy(src, dst, load_sem.at[n])
        for n, (src, dst) in enumerate([(pool_hbm, pool_ref), (q_hbm, q_ref), (dq_hbm, dq_ref)])
    ]
    for load in loads:
        load.start()

    holder = holder_ref[...]
    steps_z = lax.rem(my_z - holder // X + Z, Z)
    steps_x = lax.rem(my_x - holder % X + X, X)
    spots = (iota((LANES, pull), 0) == steps_x * Z + steps_z).astype(jnp.bfloat16)
    slot = jnp.broadcast_to((slot_ref[...] + 1).astype(jnp.float32), (8, pull)).astype(jnp.bfloat16)
    request = dot_t(slot, spots)
    c_ref[0] = request[:1]
    share = suf_ref.shape[1]
    flat = suffix_ref[...].astype(jnp.float32)
    suf_ref[0] = jnp.concatenate([flat[:, r * PAIR : (r + 1) * PAIR] for r in range(share)], axis=0).astype(
        jnp.bfloat16
    )
    pl.semaphore_wait(barrier, len(zs) + len(xs) + 1)

    c_copies = [remote(c_ref.at[0], c_ref.at[e], c_send.at[e], c_recv.at[e], at_x(-e)) for e in xs]
    for copy in c_copies:
        copy.start()
    s_copies = [remote(suf_ref.at[0], suf_ref.at[e], s_send.at[e], s_recv.at[e], at_x(e)) for e in xs]
    for copy in s_copies:
        copy.start()
    live = (request > 0.0).astype(jnp.bfloat16)
    before = (iota((LANES, LANES), 0) < iota((LANES, LANES), 1)).astype(jnp.bfloat16)
    place = dot(live, before)[:1].astype(jnp.int32)
    select = ((iota((pull, LANES), 0) == place) & (request[:1] > 0.0)).astype(jnp.bfloat16)
    loads[1].wait()
    prepare_queries(q_ref, q_first, q_second)
    for copy in c_copies:
        copy.wait_recv()
    rows = [c_ref[e] for e in range(X)]
    c_all = jnp.concatenate(rows + [jnp.zeros((LANES - X, LANES), jnp.float32)], axis=0)
    c_mine = jnp.where(iota((LANES, LANES), 1) // Z == iota((LANES, LANES), 0), c_all, 0.0).astype(jnp.bfloat16)
    pick = (iota((Z, LANES), 1) % Z == iota((Z, LANES), 0)).astype(jnp.bfloat16)
    table = dot_t(pick, c_mine)
    for d in range(Z):
        t_ref[d] = table[d : d + 1, :]

    w_copies = [remote(t_ref.at[d], w_ref.at[d], w_send.at[d], w_recv.at[d], at_z(-d)) for d in zs]
    for copy in w_copies:
        copy.start()
    w_ref[0] = t_ref[0]
    loads[0].wait()
    loads[2].wait()
    decode_rows(dlen_ref, dq_ref, pool_ref, dout_ref)
    for copy in w_copies:
        copy.wait_recv()
    spread = jnp.concatenate([jnp.broadcast_to(w_ref[d], (X, LANES)) for d in range(Z)], axis=0)
    mine = iota((Z * X, LANES), 1) == iota((Z * X, LANES), 0) % X
    wanted = jnp.sum(jnp.where(mine, spread, 0.0), axis=1, keepdims=True).astype(jnp.int32)
    gather = (wanted == iota((Z * X, pages), 1) + 1).astype(jnp.bfloat16)

    def along_z(k):
        lo, hi = spans[k]
        return [
            remote(sendz.at[d, :, lo:hi], recvz.at[d, :, lo:hi], z_send.at[k, d], z_recv.at[k, d], at_z(d)) for d in zs
        ]

    def along_x(k):
        lo, hi = spans[k]
        return [
            remote(sendx.at[e, :, lo:hi], recvx.at[e, :, lo:hi], x_send.at[k, e], x_recv.at[k, e], at_x(e)) for e in xs
        ]

    of, to = iota((X * Z, Z * X), 1), iota((X * Z, Z * X), 0)
    turn = ((of % X == to // Z) & (of // X == to % Z)).astype(jnp.bfloat16)
    back = ((of % Z == to // X) & (of // Z == to % X)).astype(jnp.bfloat16)
    orders = {"zx": (gather, select[:, : X * Z]), "xz": (None, None)}
    orders["xz"] = tuple(
        m.astype(jnp.bfloat16) for m in (dot(turn, gather), dot(select[:, : X * Z], turn))
    )

    def put_z(k, rows):
        lo, hi = spans[k]
        sendz[:, :, lo:hi] = rows.reshape(Z, X, hi - lo).astype(jnp.bfloat16)
        for copy in along_z(k):
            copy.start()
        recvz[0, :, lo:hi] = sendz[0, :, lo:hi]

    def put_x(k, rows):
        lo, hi = spans[k]
        sendx[:, :, lo:hi] = rows.reshape(X, Z, hi - lo).astype(jnp.bfloat16)
        for copy in along_x(k):
            copy.start()
        recvx[0, :, lo:hi] = sendx[0, :, lo:hi]

    def got(k, axis):
        lo, hi = spans[k]
        for copy in along_z(k) if axis == "z" else along_x(k):
            copy.wait_recv()
        ref = recvz if axis == "z" else recvx
        return ref[:, :, lo:hi].astype(jnp.float32).reshape(X * Z, hi - lo).astype(jnp.bfloat16)

    def send(k):
        lo, hi = spans[k]
        start = pl.multiple_of(my_c * half + lo, LANES)
        taken = dot(orders[ROUTES[k]][0], pool_ref[:, pl.ds(start, hi - lo)])
        (put_z if ROUTES[k] == "zx" else put_x)(k, taken)

    def pass_on(k):
        if ROUTES[k] == "zx":
            put_x(k, dot(turn, got(k, "z")))
        else:
            put_z(k, dot(back, got(k, "x")))

    def ring(k):
        lo, hi = spans[k]
        right_hops = RIGHT_HOPS[k % 4]
        left_hops = X - 1 - right_hops
        at = lambda side, s: keys.at[side, s, :, lo:hi]

        def to_right(i):
            return remote(at(0, i - 1), at(0, i), r_send.at[k, i], r_recv.at[k, i], at_x(1))

        def to_left(i):
            return remote(at(0, (X - i + 1) % X), at(0, X - i), l_send.at[k, i], l_recv.at[k, i], at_x(-1))

        def across(s):
            return remote(at(0, s), at(1, s), d_send.at[k, s], d_recv.at[k, s], sibling)

        def begin():
            keys[0, 0, :, lo:hi] = dot(orders[ROUTES[k]][1], got(k, ROUTES[k][1])).astype(jnp.bfloat16)
            if right_hops:
                to_right(1).start()
            if left_hops:
                to_left(1).start()
            across(0).start()

        def hop(i):
            if i <= right_hops:
                to_right(i).wait_recv()
                if i < right_hops:
                    to_right(i + 1).start()
                across(i).start()
            if i <= left_hops:
                to_left(i).wait_recv()
                if i < left_hops:
                    to_left(i + 1).start()
                across(X - i).start()

        def arrived():
            for s in range(X):
                across(s).wait_recv()

        def end():
            for i in range(1, right_hops + 1):
                to_right(i).wait_send()
            for i in range(1, left_hops + 1):
                to_left(i).wait_send()
            for s in range(X):
                across(s).wait_send()

        return begin, hop, arrived, end, max(right_hops, left_hops)

    rings = [ring(k) for k in range(len(spans))]
    length = len_ref[my_z]
    attend = functools.partial(
        attend_pair, X, my_x, length, keys, suf_ref, q_first, q_second, peak_ref, total_ref, acc_first, acc_second, out_ref
    )
    blocks = q_first.shape[0] // HEAD_BLOCK
    n_spans = len(spans)
    for copy in s_copies:
        copy.wait_recv()
    for step in STEPS:
        what, numbers = step[0], [int(n) for n in step[1:]]
        if what == "s":
            send(*numbers)
        elif what == "p":
            pass_on(*numbers)
        elif what == "b":
            rings[numbers[0]][0]()
        elif what == "h":
            k, i = numbers
            if i <= rings[k][4]:
                rings[k][1](i)
        elif what == "w":
            rings[numbers[0]][2]()
        elif what == "a":
            attend(*numbers)

    for copy in c_copies + w_copies + s_copies:
        copy.wait_send()
    for k in range(n_spans):
        for copy in along_z(k) + along_x(k):
            copy.wait_send()
        rings[k][3]()


def prepare_queries(q_ref, q_first, q_second):
    for hp in range(q_ref.shape[1] // PAIR):
        low = q_ref[:, hp * PAIR : hp * PAIR + WIDE]
        high = q_ref[:, hp * PAIR + LATENT_WIDTH : (hp + 1) * PAIR]
        first_low, second_low, first_high, second_high = both_forms(low, high)
        q_first[2 * hp] = first_low
        q_second[2 * hp] = second_low
        q_first[2 * hp + 1] = first_high
        q_second[2 * hp + 1] = second_high


def attend_pair(
    X, my_x, length, keys, suf_ref, q_first, q_second, peak_ref, total_ref, acc_first, acc_second, out_ref, p, b
):
    tokens = q_first.shape[1]
    rows = HEAD_BLOCK * tokens
    heads = slice(b * HEAD_BLOCK, (b + 1) * HEAD_BLOCK)
    queries = [q_first[heads].reshape(rows, WIDE), q_second[heads].reshape(rows, WIDE)]
    share = suf_ref.shape[1]
    last = p == keys.shape[3] // PAIR - 1
    pieces, places = [], []
    if p == 0:
        token = iota((rows, share * X), 0) % tokens
        lane = iota((rows, share * X), 1)
        rank = lax.rem(my_x - lane // share + X, X)
        for par in range(2):
            at = par * LATENT_WIDTH
            k = suf_ref[:, :, at : at + WIDE].astype(jnp.float32).reshape(X * share, WIDE).astype(jnp.bfloat16)
            s = dot_t(queries[par], k) * log2_scale
            pos = rank * (2 * share) + 2 * (lane % share) + par
            pieces.append(jnp.where((pos <= token) & (pos < length), s, masked_score))
            places.append(k)
    for side in range(2):
        for par in range(2):
            at = p * PAIR + par * LATENT_WIDTH
            k = keys[side, :, :, at : at + WIDE].reshape(-1, WIDE)
            pieces.append(dot_t(queries[par], k) * log2_scale)
            places.append(k)
    peak = functools.reduce(jnp.maximum, [jnp.max(s, axis=1, keepdims=True) for s in pieces])
    if p:
        old = peak_ref[b][:, :1]
        peak = jnp.maximum(peak, old)
        factor = jnp.exp2(old - peak)
        total = total_ref[b][:, :1] * factor
        acc = [acc_first[b] * factor, acc_second[b] * factor]
    else:
        total = jnp.zeros((rows, 1), jnp.float32)
        acc = [jnp.zeros((rows, LATENT_WIDTH), jnp.float32), jnp.zeros((rows, WIDE), jnp.float32)]
    for n, s in enumerate(pieces):
        par = n % 2
        powers = jnp.exp2(s - peak)
        total = total + jnp.sum(powers, axis=1, keepdims=True)
        acc[par] = acc[par] + dot(powers.astype(jnp.bfloat16), places[n][:, : LATENT_WIDTH if par == 0 else WIDE])
    if not last:
        peak_ref[b] = jnp.broadcast_to(peak, (rows, LANES))
        total_ref[b] = jnp.broadcast_to(total, (rows, LANES))
        acc_first[b] = acc[0]
        acc_second[b] = acc[1]
        return
    result = finish(acc[0], acc[1], total)
    token = iota(result.shape, 0) % tokens
    result = jnp.where(token < length, result, 0.0).astype(jnp.bfloat16)
    for h in range(HEAD_BLOCK):
        at = (b * HEAD_BLOCK + h) * LATENT_WIDTH
        out_ref[:, at : at + LATENT_WIDTH] = result[h * tokens : (h + 1) * tokens]


def decode_rows(len_ref, dq_ref, pool_ref, out_ref):
    n_rows = dq_ref.shape[0]
    pages = pool_ref.shape[0]
    row_pages = pages // n_rows
    head_pairs = dq_ref.shape[1] // PAIR
    half = n_rows * head_pairs
    flat = dq_ref[...].astype(jnp.float32)
    queries = jnp.concatenate([flat[:, n * PAIR : (n + 1) * PAIR] for n in range(head_pairs)], axis=0)
    first_low, second_low, first_high, second_high = both_forms(queries[:, :WIDE], queries[:, LATENT_WIDTH:])
    queries = [
        jnp.concatenate([first_low, first_high], axis=0),
        jnp.concatenate([second_low, second_high], axis=0),
    ]
    count = 2 * half
    page = iota((count, pages), 1)
    owner = iota((count, pages), 0) % n_rows
    limit = jnp.zeros((count, pages), jnp.int32)
    for r in range(n_rows):
        limit = jnp.where(owner == r, len_ref[r], limit)
    limit = jnp.where(page // row_pages == owner, limit, 0)
    page_tokens = pool_ref.shape[1] // KEY
    pieces = []
    for n in range(page_tokens):
        at = (n // 2) * PAIR + (n % 2) * LATENT_WIDTH
        s = dot_t(queries[n % 2], pool_ref[:, at : at + WIDE]) * log2_scale
        pieces.append(jnp.where((page % row_pages) * page_tokens + n < limit, s, masked_score))
    peak = functools.reduce(jnp.maximum, [jnp.max(s, axis=1, keepdims=True) for s in pieces])
    total = jnp.zeros((count, 1), jnp.float32)
    acc = [jnp.zeros((count, LATENT_WIDTH), jnp.float32), jnp.zeros((count, WIDE), jnp.float32)]
    for n in range(page_tokens):
        at = (n // 2) * PAIR + (n % 2) * LATENT_WIDTH
        width = LATENT_WIDTH if n % 2 == 0 else WIDE
        powers = jnp.exp2(pieces[n] - peak)
        total = total + jnp.sum(powers, axis=1, keepdims=True)
        acc[n % 2] = acc[n % 2] + dot(powers.astype(jnp.bfloat16), pool_ref[:, at : at + width])
    result = finish(acc[0], acc[1], total).astype(jnp.float32)
    for n in range(head_pairs):
        at = n * 2 * LATENT_WIDTH
        low = slice(n * n_rows, (n + 1) * n_rows)
        high = slice(half + n * n_rows, half + (n + 1) * n_rows)
        out_ref[:, at : at + LATENT_WIDTH] = result[low].astype(jnp.bfloat16)
        out_ref[:, at + LATENT_WIDTH : at + 2 * LATENT_WIDTH] = result[high].astype(jnp.bfloat16)


def hand_over(a_in, b_in, a_out, b_out, a_held, b_held, in_sem, out_sem):
    takes = [pltpu.make_async_copy(a_in, a_held, in_sem.at[0]), pltpu.make_async_copy(b_in, b_held, in_sem.at[1])]
    gives = [pltpu.make_async_copy(a_held, a_out, out_sem.at[0]), pltpu.make_async_copy(b_held, b_out, out_sem.at[1])]
    for copy in takes:
        copy.start()
    for take, give in zip(takes, gives):
        take.wait()
        give.start()
    for copy in gives:
        copy.wait()


def shards(
    Z,
    X,
    pool,
    page_holder,
    page_slot,
    suffix_latent_rows,
    prefill_queries,
    suffix_len,
    decode_queries,
    decode_len,
):
    pages = pool.shape[0]
    pull = page_holder.shape[0]
    half = pool.shape[1] // 2
    tokens = prefill_queries.shape[1]
    heads = prefill_queries.shape[2] // KEY
    decode_heads = decode_queries.shape[1] // KEY
    share = suffix_latent_rows.shape[1] // PAIR
    n_spans = 2 * half // PAIR
    blocks = heads // HEAD_BLOCK
    rows = HEAD_BLOCK * tokens
    bf16, f32 = jnp.bfloat16, jnp.float32
    hbm, vmem, smem = (pl.BlockSpec(memory_space=m) for m in (pl.ANY, pltpu.VMEM, pltpu.SMEM))
    dma = pltpu.SemaphoreType.DMA
    prefill_part, decode_part = pl.pallas_call(
        functools.partial(kernel, Z, X),
        out_shape=(
            jax.ShapeDtypeStruct((tokens, heads * LATENT_WIDTH), bf16),
            jax.ShapeDtypeStruct((decode_queries.shape[0], decode_heads * LATENT_WIDTH), bf16),
        ),
        in_specs=[hbm, hbm, hbm, vmem, vmem, vmem, smem, smem],
        out_specs=(vmem, vmem),
        scratch_shapes=[
            pltpu.VMEM(pool.shape, bf16),
            pltpu.VMEM((tokens, heads * KEY), bf16),
            pltpu.VMEM(decode_queries.shape, bf16),
            pltpu.VMEM((X, 1, LANES), f32),
            pltpu.VMEM((Z, 1, LANES), f32),
            pltpu.VMEM((Z, 1, LANES), f32),
            pltpu.VMEM((X, share, PAIR), bf16),
            pltpu.VMEM((Z, X, half), bf16),
            pltpu.VMEM((Z, X, half), bf16),
            pltpu.VMEM((X, Z, half), bf16),
            pltpu.VMEM((X, Z, half), bf16),
            pltpu.VMEM((2, X, pull, half), bf16),
            pltpu.VMEM((heads, tokens, WIDE), bf16),
            pltpu.VMEM((heads, tokens, WIDE), bf16),
            pltpu.VMEM((blocks, rows, LANES), f32),
            pltpu.VMEM((blocks, rows, LANES), f32),
            pltpu.VMEM((blocks, rows, LATENT_WIDTH), f32),
            pltpu.VMEM((blocks, rows, WIDE), f32),
            dma((3,)),
            dma((X,)),
            dma((X,)),
            dma((Z,)),
            dma((Z,)),
            dma((X,)),
            dma((X,)),
            dma((n_spans, Z)),
            dma((n_spans, Z)),
            dma((n_spans, X)),
            dma((n_spans, X)),
            dma((n_spans, X)),
            dma((n_spans, X)),
            dma((n_spans, X)),
            dma((n_spans, X)),
            dma((n_spans, X)),
            dma((n_spans, X)),
        ],
        compiler_params=pltpu.CompilerParams(
            collective_id=0, has_side_effects=True, vmem_limit_bytes=60 * 1024 * 1024
        ),
        name="whole",
    )(
        pool,
        prefill_queries[0],
        decode_queries,
        page_holder[None],
        page_slot[None],
        suffix_latent_rows,
        suffix_len,
        decode_len,
    )
    prefill_part, decode_part = pl.pallas_call(
        hand_over,
        out_shape=tuple(jax.ShapeDtypeStruct(a.shape, a.dtype) for a in (prefill_part, decode_part)),
        in_specs=[hbm, hbm],
        out_specs=(hbm, hbm),
        scratch_shapes=[
            pltpu.VMEM(prefill_part.shape, bf16),
            pltpu.VMEM(decode_part.shape, bf16),
            dma((2,)),
            dma((2,)),
        ],
        compiler_params=pltpu.CompilerParams(vmem_limit_bytes=60 * 1024 * 1024),
        name="hand_over",
    )(prefill_part, decode_part)
    return (prefill_part[None], decode_part)


def solution(mesh):
    groups, dp, tp = (mesh.shape[name] for name in ("groups", "dp", "tp"))
    X = TEAM_RANKS
    Z = dp // X
    torus = Mesh(mesh.devices.reshape(groups, Z, X, tp), ("groups", "dp_0", "dp_1", "tp"))
    placed = (
        P(GROUPS_DP, None),
        P(GROUPS_DP),
        P(GROUPS_DP),
        P(GROUPS_DP, None),
        P(GROUPS_DP, None, "tp"),
        P("groups"),
        P(GROUPS_DP, "tp"),
        P(GROUPS_DP),
    )
    return jax.shard_map(
        functools.partial(shards, Z, X),
        mesh=torus,
        in_specs=placed,
        out_specs=(P(GROUPS_DP, None, "tp"), P(GROUPS_DP, "tp")),
        check_vma=False,
    )
```
